32 devices in a mesh: blk: 2 (over x), wide: 16 (over z, y, core).
Axes of the slice: x: 2, y: 2, z: 4, core: 2. Of those that a mesh axis runs over, the one named last changes fastest.
Arguments:
- volume: float32 [2, 2, 512, 896], P('blk', None, 'wide'), may hold values from -1.6 to 1.6
- path_lengths: float32 [2, 2, 2], replicated, may hold values from 0.5 to 2
- probe: float32 [2, 128, 128], replicated, may hold values from -6 to 6
- measured: bfloat16 [2, 16, 14, 128, 128], P('blk', 'wide'), may hold values from 0.19921875 to 3
- jitter: int32 [2, 2, 16, 14], P(None, 'blk', 'wide'), may hold values from 0 to 15
- step_sizes: float32 [2], replicated, may hold values from 0.02 to 0.2
Outputs:
- new_volume: float32 [2, 2, 512, 896], P('blk', None, 'wide')
- misfit: float32 [], replicated
The draws below stay inside these ranges and needn't reach their ends.
All inputs are finite; a program needn't handle non-finite values.
Results may differ from the reference program's by a relative error of at most 0.0003.
Values sent between devices are 32-bit elements; how exact they have to be, the bound alone decides.
No kernel may reach another device: no remote copies, remote signals or barrier semaphores. Data moves between devices by JAX's collectives and lax.ppermute only.
A program may use at most 64 MiB of HBM per device.

```python
import math
import jax
import jax.numpy as jnp
from jax import lax

LAYERS = 2
ROWS_DEV = 32
COLS = 896
PATCH = 128
CSTEP = 64
JIT = 16
PCOLS = 14
HEIGHT = 512
N_BLK = 2
N_WIDE = 16


def with_ends(drawn, stream_key, least, largest):
    extent = drawn.shape
    spot = [jax.random.randint(jax.random.fold_in(stream_key, axis), (), 0, extent[axis]) for axis in range(len(extent))]
    drawn = drawn.at[tuple(spot)].set(least)
    longest = extent.index(max(extent))
    spot[longest] = (spot[longest] + 1) % extent[longest]
    return drawn.at[tuple(spot)].set(largest)


def shard_levels(rng, dims, pieces, smallest, top_value):
    loudness, own = 1.0, jax.random.fold_in(rng, 6)
    for dim, shards_of in pieces:
        draws = jnp.exp(jax.random.uniform(jax.random.fold_in(own, dim), (shards_of,), jnp.float32, smallest / len(pieces), top_value / len(pieces)))
        loudness = loudness * jnp.repeat(draws, dims[dim] // shards_of).reshape([-1 if axis == dim else 1 for axis in range(len(dims))])
    return loudness


def noise(key, dims, scale, bound, shards=(), kind=jnp.bfloat16):
    drawn = jax.random.normal(key, dims, jnp.float32) * scale
    if len(shards) > 0:
        drawn = shard_levels(key, dims, shards, -0.22, 0.18) * drawn
    return jnp.clip(drawn, min=-bound, max=bound).astype(kind)


def setup_inputs(seed: int = 0) -> dict:
    streams_of = jax.random.split(jax.random.key(seed), 7)
    return {
        "volume": noise(streams_of[0], (N_BLK, LAYERS, HEIGHT, COLS), 0.2, 1.6, ((0, 2), (2, 16)), jnp.float32),
        "path_lengths": jnp.clip(jnp.exp(jax.random.uniform(streams_of[1], (N_BLK, N_BLK, LAYERS), jnp.float32, math.log(0.5), math.log(2.0))), 0.5, 2.0),
        "probe": noise(streams_of[2], (2, PATCH, PATCH), 1.0, 6.0, (), jnp.float32),
        "measured": jnp.clip(jnp.exp(math.log(3.0) - 2.7119641 * jax.random.uniform(streams_of[3], (N_BLK, N_WIDE, PCOLS, PATCH, PATCH), jnp.float32) ** shard_levels(streams_of[3], (N_BLK, N_WIDE, PCOLS, PATCH, PATCH), ((0, 2), (1, 16)), -0.2, 0.2)), 0.19921875, 3.0).astype(jnp.bfloat16),
        "jitter": with_ends(jax.random.randint(streams_of[4], (2, N_BLK, N_WIDE, PCOLS), 0, JIT), jax.random.fold_in(streams_of[4], 1), 0, JIT - 1).astype(jnp.int32),
        "step_sizes": jnp.clip(jnp.exp(jax.random.uniform(streams_of[5], (N_BLK,), jnp.float32, math.log(0.02), math.log(0.2))), 0.02, 0.2),
    }


highest = lax.Precision.HIGHEST
floor_value = 0.25

def dft_tables(length):
    grid = jnp.arange(length, dtype=jnp.int32)
    product = grid[:, None] * grid[None, :] % length
    angles = product.astype(jnp.float32) * (2.0 * math.pi / length)
    factor = 1.0 / math.sqrt(length)
    return (jnp.cos(angles) * factor, -jnp.sin(angles) * factor)

def left_apply(table, batch):
    return jnp.einsum('jk,bkl->bjl', table, batch, precision=highest)

def right_apply(batch, table):
    return jnp.einsum('bjk,kl->bjl', batch, table, precision=highest)

def transform(real_in, imag_in, cos_table, sin_table):
    mid_real = left_apply(cos_table, real_in) - left_apply(sin_table, imag_in)
    mid_imag = left_apply(cos_table, imag_in) + left_apply(sin_table, real_in)
    out_real = right_apply(mid_real, cos_table) - right_apply(mid_imag, sin_table)
    out_imag = right_apply(mid_real, sin_table) + right_apply(mid_imag, cos_table)
    return (out_real, out_imag)

def strip_update(strip_real, strip_imaginary, probe, measured, jitter_rows, jitter_cols, row_corner, column_corner):
    patch_len = probe.shape[-1]
    number = measured.shape[0]
    cos_table, sin_table = dft_tables(patch_len)
    starts_row = (row_corner + jitter_rows).astype(jnp.int32)
    starts_col = (column_corner + CSTEP * jnp.arange(number, dtype=jnp.int32) + jitter_cols).astype(jnp.int32)

    def window(image, top, left):
        return lax.dynamic_slice(image, (top, left), (patch_len, patch_len))
    pick = jax.vmap(window, in_axes=(None, 0, 0))
    obj_real = pick(strip_real, starts_row, starts_col)
    obj_imag = pick(strip_imaginary, starts_row, starts_col)
    probe_real = probe[0]
    probe_imag = probe[1]
    wave_real = probe_real * obj_real - probe_imag * obj_imag
    wave_imag = probe_real * obj_imag + probe_imag * obj_real
    far_real, far_imag = transform(wave_real, wave_imag, cos_table, sin_table)
    modulus = jnp.sqrt(far_real * far_real + far_imag * far_imag)
    target = measured.astype(jnp.float32)
    error = modulus - target
    partial_misfit = jnp.sum(error * error)
    ratio = target / jnp.maximum(modulus, floor_value)
    back_real, back_imag = transform(ratio * far_real, ratio * far_imag, cos_table, -sin_table)
    diff_real = back_real - wave_real
    diff_imag = back_imag - wave_imag
    corr_real = probe_real * diff_real + probe_imag * diff_imag
    corr_imag = probe_real * diff_imag - probe_imag * diff_real

    def place(position, sums):
        acc_real, acc_imag = sums
        top = starts_row[position]
        left = starts_col[position]
        acc_real = lax.dynamic_update_slice(acc_real, window(acc_real, top, left) + corr_real[position], (top, left))
        acc_imag = lax.dynamic_update_slice(acc_imag, window(acc_imag, top, left) + corr_imag[position], (top, left))
        return (acc_real, acc_imag)
    zeros = jnp.zeros(strip_real.shape, strip_real.dtype)
    acc_real, acc_imag = lax.fori_loop(0, number, place, (zeros, zeros))
    return (acc_real, acc_imag, partial_misfit)

def reference(volume, path_lengths, probe, measured, jitter, step_sizes):
    projections = jnp.einsum('asl,slhc->ahc', path_lengths, volume, precision=highest)
    margin = PATCH // 2
    row_corner = ROWS_DEV // 4
    column_corner = PATCH // 4 - ROWS_DEV // 4
    height = ROWS_DEV * N_WIDE
    band_rows = 5 * ROWS_DEV
    gradients = []
    total = jnp.zeros((), jnp.float32)
    for angle in range(N_BLK):
        phase = projections[angle]
        obj_real = jnp.pad(jnp.cos(phase), ((2 * ROWS_DEV, 2 * ROWS_DEV), (margin, margin)))
        obj_imag = jnp.pad(jnp.sin(phase), ((2 * ROWS_DEV, 2 * ROWS_DEV), (margin, margin)))
        width_all = obj_real.shape[1]

        def row_step(carry, input_arrays):
            acc_real, acc_imag, running = carry
            strip_index, recorded_row, shaken_rows, shaken_columns = input_arrays
            top = (strip_index * ROWS_DEV).astype(jnp.int32)
            zero_col = jnp.zeros((), jnp.int32)
            strip_real = lax.dynamic_slice(obj_real, (top, zero_col), (band_rows, width_all))
            strip_imaginary = lax.dynamic_slice(obj_imag, (top, zero_col), (band_rows, width_all))
            portion_real, portion_imaginary, part = strip_update(strip_real, strip_imaginary, probe, recorded_row, shaken_rows, shaken_columns, row_corner, column_corner)
            acc_real = lax.dynamic_update_slice(acc_real, lax.dynamic_slice(acc_real, (top, zero_col), (band_rows, width_all)) + portion_real, (top, zero_col))
            acc_imag = lax.dynamic_update_slice(acc_imag, lax.dynamic_slice(acc_imag, (top, zero_col), (band_rows, width_all)) + portion_imaginary, (top, zero_col))
            return ((acc_real, acc_imag, running + part), None)
        input_arrays = (jnp.arange(N_WIDE, dtype=jnp.int32), measured[angle], jitter[0, angle], jitter[1, angle])
        start = (jnp.zeros(obj_real.shape, jnp.float32), jnp.zeros(obj_real.shape, jnp.float32), jnp.zeros((), jnp.float32))
        (acc_real, acc_imag, part), unused = lax.scan(row_step, start, input_arrays)
        total = total + part
        inner_r = slice(2 * ROWS_DEV, 2 * ROWS_DEV + height)
        inner_c = slice(margin, margin + COLS)
        gradients.append(obj_real[inner_r, inner_c] * acc_imag[inner_r, inner_c] - obj_imag[inner_r, inner_c] * acc_real[inner_r, inner_c])
    stacked = jnp.stack(gradients, 0)
    coeffs = step_sizes[:, None, None] * path_lengths
    update = jnp.einsum('asl,ahc->slhc', coeffs, stacked, precision=highest)
    return (volume - update, total)
```

```python
import functools
import math

import jax
import jax.numpy as jnp
import numpy as np
from jax import lax
from jax.experimental import pallas as pl
from jax.experimental.pallas import tpu as pltpu
from jax.sharding import PartitionSpec as P

ROWS_DEV = 32
CSTEP = 64
JIT = 16
FLOOR_RATIO = 4.0
LANES = 128
SUBS = 8
HALF_PI = (1.5703125, 4.837512969970703125e-4, 7.54978995489188216e-8)


def dft_tables(length):
    grid = np.arange(length)
    angles = (grid[:, None] * grid[None, :] % length) * (2.0 * math.pi / length)
    cos = np.cos(angles) / math.sqrt(length)
    sin = -np.sin(angles) / math.sqrt(length)
    table = np.block([[cos, sin], [-sin, cos]])
    high = table.astype(jnp.bfloat16)
    low = (table - high.astype(np.float64)).astype(jnp.bfloat16)
    right = lambda h, l: np.concatenate([h, h, l], 0)
    left = lambda h, l: np.concatenate([h, h, l], 1)
    return right(high, low), left(high.T, low.T), left(high, low), right(high.T, low.T)


def sin_cos(x):
    turns = jnp.floor(x * (2.0 / math.pi) + 0.5)
    r = x - turns * HALF_PI[0]
    r = r - turns * HALF_PI[1]
    r = r - turns * HALF_PI[2]
    quadrant = turns.astype(jnp.int32)
    z = r * r
    s = r + r * z * (-1.6666654611e-1 + z * (8.3321608736e-3 + z * -1.9515295891e-4))
    c = 1.0 - 0.5 * z + z * z * (
        4.166664568298827e-2 + z * (-1.388731625493765e-3 + z * 2.443315711809948e-5)
    )
    odd = (quadrant & 1) == 1
    sin = jnp.where(odd, c, s)
    cos = jnp.where(odd, s, c)
    sin = jnp.where((quadrant & 2) == 2, -sin, sin)
    cos = jnp.where(((quadrant + 1) & 2) == 2, -cos, cos)
    return sin, cos


def parts_of(x):
    high = x.astype(jnp.bfloat16)
    low = (x - high.astype(jnp.float32)).astype(jnp.bfloat16)
    return high, low


def window_place(position, patch):
    corner = patch // 4 - ROWS_DEV // 4 - patch // 2 + CSTEP * position
    tile = corner // LANES
    return tile, corner - tile * LANES


def strip_kernel(
    far,
    jitter,
    ends,
    own,
    mate,
    cross,
    relay,
    probe,
    measured,
    fwd_right,
    fwd_left,
    inv_left,
    inv_right,
    grad,
    misfit,
    obj_real,
    obj_imag,
    wave,
    twice,
    mid,
    back,
):
    number, patch, _ = measured.shape
    rows = own.shape[0]
    tiles = own.shape[1] // LANES
    near = ROWS_DEV // 4 + JIT
    dot = functools.partial(lax.dot, preferred_element_type=jnp.float32)

    is_odd = ends[0] == 1
    odd = jnp.full((SUBS, LANES), ends[0], jnp.int32) == 1
    up2_ok = ends[1].astype(jnp.float32)
    up1_ok = ends[2].astype(jnp.float32)
    dn1_ok = ends[3].astype(jnp.float32)
    dn2_ok = ends[4].astype(jnp.float32)

    for half in range(2):
        twice[0, half * patch : (half + 1) * patch, :] = probe[0]
        twice[1, half * patch : (half + 1) * patch, :] = probe[1]

    def put(row, phase, ok):
        s, c = sin_cos(phase)
        if ok is not None:
            s = s * ok
            c = c * ok
        obj_real[row : row + SUBS, :] = c
        obj_imag[row : row + SUBS, :] = s

    for r in range(0, rows, SUBS):
        put(2 * rows + r, own[r : r + SUBS, :], None)
    wide_odd = jnp.full((SUBS, own.shape[1]), ends[0], jnp.int32) == 1
    for r in range(0, far, SUBS):
        top = rows - far + r
        put(top, jnp.where(wide_odd, relay[r : r + SUBS, :], cross[r : r + SUBS, :]), up2_ok)
    for r in range(0, rows, SUBS):
        put(rows + r, jnp.where(wide_odd, mate[r : r + SUBS, :], cross[far + r : far + r + SUBS, :]), up1_ok)
    for r in range(0, rows, SUBS):
        put(3 * rows + r, jnp.where(wide_odd, cross[r : r + SUBS, :], mate[r : r + SUBS, :]), dn1_ok)
    for r in range(0, far, SUBS):
        put(4 * rows + r, jnp.where(wide_odd, cross[rows + r : rows + r + SUBS, :], relay[r : r + SUBS, :]), dn2_ok)

    lane = lax.broadcasted_iota(jnp.int32, (SUBS, LANES), 1)
    sub = lax.broadcasted_iota(jnp.int32, (SUBS, LANES), 0)

    def first_row(p):
        return ROWS_DEV // 4 + jitter[0, p]

    def masks(p):
        _, corner = window_place(p, patch)
        after = lane >= corner + jitter[1, p]
        below = [sub + k * SUBS >= first_row(p) for k in range(near // SUBS)]
        return after, below

    def pick(ref, p, k, after, below):
        tile, _ = window_place(p, patch)

        def at(row):
            left = ref[row : row + SUBS, tile * LANES : (tile + 1) * LANES] if tile >= 0 else 0.0
            right = (
                ref[row : row + SUBS, (tile + 1) * LANES : (tile + 2) * LANES]
                if tile + 1 < tiles
                else 0.0
            )
            return jnp.where(after, left, right)

        row = k * SUBS
        if row + SUBS <= ROWS_DEV // 4:
            return at(row + patch)
        if row < near:
            return jnp.where(below[k], at(row), at(row + patch))
        return at(row)

    steps = patch // SUBS
    for p in range(number):
        after, below = masks(p)
        _, corner = window_place(p, patch)
        shift = corner + jitter[1, p]
        start = patch - first_row(p)
        p_real = pltpu.roll(twice[0, pl.ds(start, patch), :], shift, 1)
        p_imag = pltpu.roll(twice[1, pl.ds(start, patch), :], shift, 1)
        for k in range(steps):
            o_real = pick(obj_real, p, k, after, below)
            o_imag = pick(obj_imag, p, k, after, below)
            a = p_real[k * SUBS : (k + 1) * SUBS]
            b = p_imag[k * SUBS : (k + 1) * SUBS]
            row = p * patch + k * SUBS
            wave[row : row + SUBS, :LANES] = a * o_real - b * o_imag
            wave[row : row + SUBS, LANES:] = a * o_imag + b * o_real

    for p in range(0, number, 2):
        high, low = parts_of(wave[p * patch : (p + 2) * patch, :])
        mid[p * patch : (p + 2) * patch, :] = dot(jnp.concatenate([high, low, high], 1), fwd_right[...])

    def upright(value):
        top = jnp.concatenate([value[:patch, :LANES], value[patch:, :LANES]], 1)
        low = jnp.concatenate([value[:patch, LANES:], value[patch:, LANES:]], 1)
        return jnp.concatenate([top, low], 0)

    total = jnp.zeros((SUBS, LANES), jnp.float32)
    for p in range(0, number, 2):
        high, low = parts_of(upright(mid[p * patch : (p + 2) * patch, :]))
        spectrum = dot(fwd_left[...], jnp.concatenate([high, low, high], 0))
        real, imag = spectrum[:patch], spectrum[patch:]
        target = jnp.concatenate([measured[p], measured[p + 1]], 1).astype(jnp.float32)
        power = real * real + imag * imag
        inverse = lax.rsqrt(jnp.maximum(power, 1e-30))
        error = power * inverse - target
        square = error * error
        for k in range(steps):
            for half in range(2):
                total += square[k * SUBS : (k + 1) * SUBS, half * LANES : (half + 1) * LANES]
        ratio = target * jnp.minimum(inverse, FLOOR_RATIO)
        high, low = parts_of(jnp.concatenate([ratio * real, ratio * imag], 0))
        undone = dot(inv_left[...], jnp.concatenate([high, low, high], 0))
        for half in range(2):
            row = (p + half) * patch
            lanes = slice(half * LANES, (half + 1) * LANES)
            back[row : row + patch, :LANES] = undone[:patch, lanes]
            back[row : row + patch, LANES:] = undone[patch:, lanes]
    misfit[...] = total

    for p in range(0, number, 2):
        high, low = parts_of(back[p * patch : (p + 2) * patch, :])
        out = dot(jnp.concatenate([high, low, high], 1), inv_right[...])
        w = wave[p * patch : (p + 2) * patch, :]
        mid[p * patch : (p + 2) * patch, :LANES] = w[:, :LANES] * out[:, LANES:] - w[:, LANES:] * out[:, :LANES]

    for t in range(tiles):
        meets = []
        for p in range(number):
            tile, _ = window_place(p, patch)
            if t in (tile, tile + 1):
                after, below = masks(p)
                meets.append((p, after if t == tile else jnp.logical_not(after), below))
        cols = slice(t * LANES, (t + 1) * LANES)
        for k in range(steps):
            row = k * SUBS
            here = there = None
            for p, mask, below in meets:
                term = jnp.where(mask, mid[p * patch + row : p * patch + row + SUBS, :LANES], 0.0)
                if row + SUBS <= ROWS_DEV // 4:
                    there = term if there is None else there + term
                elif row < near:
                    kept = jnp.where(below[k], term, 0.0)
                    here = kept if here is None else here + kept
                    there = (term - kept) if there is None else there + (term - kept)
                else:
                    here = term if here is None else here + term
            if here is not None:
                grad[row : row + SUBS, cols] = here
            else:
                grad[row : row + SUBS, cols] = jnp.zeros((SUBS, LANES), jnp.float32)
            if there is not None:
                grad[row + patch : row + patch + SUBS, cols] = there
    for row in range(patch + near, 5 * rows, SUBS):
        grad[row : row + SUBS, :] = jnp.zeros((SUBS, grad.shape[1]), jnp.float32)


def strip_gradient(far, jitter, ends, own, mate, cross, relay, probe, measured):
    number, patch, _ = measured.shape
    rows, cols = own.shape
    tables = dft_tables(patch)
    vmem = pl.BlockSpec(memory_space=pltpu.VMEM)
    smem = pl.BlockSpec(memory_space=pltpu.SMEM)
    f32 = jnp.float32
    return pl.pallas_call(
        functools.partial(strip_kernel, far),
        out_shape=(
            jax.ShapeDtypeStruct((5 * rows, cols), f32),
            jax.ShapeDtypeStruct((SUBS, LANES), f32),
        ),
        in_specs=[smem, smem] + [vmem] * 10,
        out_specs=(vmem, vmem),
        scratch_shapes=[
            pltpu.VMEM((5 * rows, cols), f32),
            pltpu.VMEM((5 * rows, cols), f32),
            pltpu.VMEM((number * patch, 2 * LANES), f32),
            pltpu.VMEM((2, 2 * patch, patch), f32),
            pltpu.VMEM((number * patch, 2 * LANES), f32),
            pltpu.VMEM((number * patch, 2 * LANES), f32),
        ],
        compiler_params=pltpu.CompilerParams(vmem_limit_bytes=40 * 1024 * 1024),
        cost_estimate=pl.CostEstimate(
            flops=24 * number * patch**3 * 4, bytes_accessed=4 * number * patch * patch, transcendentals=0
        ),
        name="strip",
    )(jitter, ends, own, mate, cross, relay, probe, measured, *tables)


def permuted(value, axis, target):
    count = lax.axis_size(axis)
    pairs = [(i, target(i)) for i in range(count) if 0 <= target(i) < count]
    return lax.ppermute(value, axis, pairs)


def with_mate(value):
    return permuted(value, "wide", lambda i: i ^ 1)


def across(value):
    return permuted(value, "wide", lambda i: i + 1 if i % 2 else i - 1)


def summed(value, axis):
    count = lax.axis_size(axis)
    if count & (count - 1):
        return lax.psum(value, axis)
    step = 1
    while step < count:
        value = value + permuted(value, axis, lambda i: i ^ step)
        step *= 2
    return value


def body(volume, path_lengths, probe, measured, jitter, step_sizes):
    group = lax.axis_index("blk")
    groups = lax.axis_size("blk")
    column = lax.axis_index("wide")
    columns = lax.axis_size("wide")
    slab = volume[0]
    rows = slab.shape[1]
    far = rows - ROWS_DEV // 4
    own_paths = lax.dynamic_index_in_dim(path_lengths, group, 1, keepdims=False)

    def slab_term(angle):
        coeffs = lax.dynamic_index_in_dim(own_paths, angle, 0, keepdims=False)
        return jnp.sum(coeffs[:, None, None] * slab, 0)

    def to_group(value, step):
        return lax.ppermute(value, "blk", [(i, (i + step) % groups) for i in range(groups)])

    own = slab_term(group)
    for step in range(1, groups):
        own = own + to_group(slab_term((group + step) % groups), step)

    odd = column % 2 == 1
    mate = with_mate(own)
    cross = across(
        jnp.where(
            odd,
            jnp.concatenate([mate[rows - far :], own], 0),
            jnp.concatenate([own, mate[:far]], 0),
        )
    )
    relay = with_mate(jnp.where(odd, cross[:far], cross[rows:]))
    ends = jnp.stack(
        [
            column % 2,
            (column >= 2).astype(jnp.int32),
            (column >= 1).astype(jnp.int32),
            (column + 1 < columns).astype(jnp.int32),
            (column + 2 < columns).astype(jnp.int32),
        ]
    )
    part, local = strip_gradient(
        far, jitter[:, 0, 0], ends, own, mate, cross, relay, probe, measured[0, 0]
    )
    up2 = part[rows - far : rows]
    up1 = part[rows : 2 * rows]
    mine = part[2 * rows : 3 * rows]
    dn1 = part[3 * rows : 4 * rows]
    dn2 = part[4 * rows : 4 * rows + far]

    def tail(value):
        return jnp.pad(value, ((rows - far, 0), (0, 0)))

    def head(value):
        return jnp.pad(value, ((0, rows - far), (0, 0)))

    got = with_mate(jnp.where(odd, up2, dn2))
    met = across(
        jnp.where(
            odd,
            jnp.concatenate([dn1 + head(got), dn2], 0),
            jnp.concatenate([up2, up1 + tail(got)], 0),
        )
    )
    last = with_mate(jnp.where(odd, up1 + tail(met[:far]), dn1 + head(met[rows:])))
    gradient = mine + last + jnp.where(odd, met[far:], met[:rows])
    total = jnp.sum(summed(summed(local, "wide"), "blk"))

    def share(angle, grad):
        coeffs = lax.dynamic_index_in_dim(own_paths, angle, 0, keepdims=False)
        scale = lax.dynamic_index_in_dim(step_sizes, angle, 0, keepdims=False)
        return (coeffs * scale)[:, None, None] * grad[None]

    update = share(group, gradient)
    for step in range(1, groups):
        update = update + share((group - step) % groups, to_group(gradient, step))
    return ((slab - update)[None], total)


def solution(mesh):
    in_specs = (
        P("blk", None, "wide", None),
        P(),
        P(),
        P("blk", "wide", None, None, None),
        P(None, "blk", "wide", None),
        P(),
    )
    out_specs = (P("blk", None, "wide", None), P())
    return jax.shard_map(body, mesh=mesh, in_specs=in_specs, out_specs=out_specs, check_vma=False)
```

```python
import functools
import math

import jax
import jax.numpy as jnp
import numpy as np
from jax import lax
from jax.experimental import pallas as pl
from jax.experimental.pallas import tpu as pltpu
from jax.sharding import PartitionSpec as P

ROWS_DEV = 32
CSTEP = 64
JIT = 16
FLOOR_RATIO = 4.0
LANES = 128
SUBS = 8
HALF_PI = (1.5703125, 4.837512969970703125e-4, 7.54978995489188216e-8)


def dft_tables(length):
    grid = np.arange(length)
    angles = (grid[:, None] * grid[None, :] % length) * (2.0 * math.pi / length)
    cos = np.cos(angles) / math.sqrt(length)
    sin = -np.sin(angles) / math.sqrt(length)
    table = np.block([[cos, sin], [-sin, cos]])
    high = table.astype(jnp.bfloat16)
    low = (table - high.astype(np.float64)).astype(jnp.bfloat16)
    return np.stack([high, low, high.T, low.T])


def sin_cos(x):
    turns = jnp.floor(x * (2.0 / math.pi) + 0.5)
    r = x - turns * HALF_PI[0]
    r = r - turns * HALF_PI[1]
    r = r - turns * HALF_PI[2]
    quadrant = turns.astype(jnp.int32)
    z = r * r
    s = r + r * z * (-1.6666654611e-1 + z * (8.3321608736e-3 + z * -1.9515295891e-4))
    c = 1.0 - 0.5 * z + z * z * (
        4.166664568298827e-2 + z * (-1.388731625493765e-3 + z * 2.443315711809948e-5)
    )
    odd = (quadrant & 1) == 1
    sin = jnp.where(odd, c, s)
    cos = jnp.where(odd, s, c)
    sin = jnp.where((quadrant & 2) == 2, -sin, sin)
    cos = jnp.where(((quadrant + 1) & 2) == 2, -cos, cos)
    return sin, cos


def parts_of(x):
    high = x.astype(jnp.bfloat16)
    low = (x - high.astype(jnp.float32)).astype(jnp.bfloat16)
    return high, low


def window_place(position, patch):
    corner = patch // 4 - ROWS_DEV // 4 - patch // 2 + CSTEP * position
    tile = corner // LANES
    return tile, corner - tile * LANES


def terms_kernel(groups, slab, paths, jitter, steps, *outs):
    terms, factors, scalars = outs[:groups], outs[groups], outs[groups + 1]
    group = lax.axis_index("blk")
    column = lax.axis_index("wide")
    columns = lax.axis_size("wide")
    layers, rows, _ = slab.shape
    for step in range(groups):
        angle = lax.rem(group + step, groups)
        for r in range(0, rows, SUBS):
            sums = slab[0, r : r + SUBS, :] * paths[angle, group, 0]
            for layer in range(1, layers):
                sums = sums + slab[layer, r : r + SUBS, :] * paths[angle, group, layer]
            terms[step][r : r + SUBS, :] = sums
        source = lax.rem(group - step + groups, groups)
        for layer in range(layers):
            factors[step, layer] = jnp.full((SUBS, LANES), steps[source] * paths[source, group, layer], jnp.float32)
    number = jitter.shape[1]
    for p in range(number):
        scalars[0, p] = jitter[0, p]
        scalars[1, p] = jitter[1, p]
        scalars[2, p] = 0
    scalars[2, 0] = lax.rem(column, 2)
    scalars[2, 1] = lax.rem(column // 2, 2)
    scalars[2, 2] = (column >= 2).astype(jnp.int32)
    scalars[2, 3] = (column >= 1).astype(jnp.int32)
    scalars[2, 4] = (column + 1 < columns).astype(jnp.int32)
    scalars[2, 5] = (column + 2 < columns).astype(jnp.int32)


def slab_terms(slab, paths, jitter, steps, groups):
    layers, rows, cols = slab.shape
    vmem = pl.BlockSpec(memory_space=pltpu.VMEM)
    smem = pl.BlockSpec(memory_space=pltpu.SMEM)
    f32 = jnp.float32
    term = jax.ShapeDtypeStruct((rows, cols), f32)
    out = pl.pallas_call(
        functools.partial(terms_kernel, groups),
        out_shape=[term] * groups
        + [
            jax.ShapeDtypeStruct((groups, layers, SUBS, LANES), f32),
            jax.ShapeDtypeStruct((3, jitter.shape[1]), jnp.int32),
        ],
        in_specs=[vmem, smem, smem, smem],
        out_specs=[vmem] * (groups + 1) + [smem],
        name="terms",
    )(slab, paths, jitter, steps)
    return out[:groups], out[groups], out[groups + 1]


def update_kernel(slab, factors, *refs):
    grads, out = refs[:-1], refs[-1]
    layers, rows, cols = slab.shape
    for layer in range(layers):
        for r in range(0, rows, SUBS):
            for c in range(0, cols, LANES):
                value = slab[layer, r : r + SUBS, c : c + LANES]
                for step, grad in enumerate(grads):
                    value = value - factors[step, layer] * grad[r : r + SUBS, c : c + LANES]
                out[layer, r : r + SUBS, c : c + LANES] = value


def updated(slab, factors, grads):
    vmem = pl.BlockSpec(memory_space=pltpu.VMEM)
    return pl.pallas_call(
        update_kernel,
        out_shape=jax.ShapeDtypeStruct(slab.shape, slab.dtype),
        in_specs=[vmem] * (2 + len(grads)),
        out_specs=vmem,
        compiler_params=pltpu.CompilerParams(vmem_limit_bytes=8 * 1024 * 1024),
        name="update",
    )(slab, factors, *grads)


def strip_kernel(
    scalars,
    own,
    mate,
    pair,
    next_pair,
    relay,
    probe,
    measured,
    tables,
    mine,
    to_mate,
    by_pair,
    by_next,
    obj_real,
    obj_imag,
    grad,
    wave,
    twice,
    mid,
    back,
):
    number, patch, _ = measured.shape
    rows, cols = own.shape
    tiles = cols // LANES
    far = rows - ROWS_DEV // 4
    near = ROWS_DEV // 4 + JIT
    dot = functools.partial(lax.dot, preferred_element_type=jnp.float32)
    jitter = scalars

    def flag(index):
        return jnp.full((SUBS, cols), scalars[2, index], jnp.int32) == 1

    is_second = flag(0)
    is_lower = flag(1)
    fwd_high, fwd_low, inv_high, inv_low = (tables[i] for i in range(4))

    for half in range(2):
        twice[0, half * patch : (half + 1) * patch, :] = probe[0]
        twice[1, half * patch : (half + 1) * patch, :] = probe[1]

    def put(row, phase, index):
        s, c = sin_cos(phase)
        if index is not None:
            ok = scalars[2, index].astype(jnp.float32)
            s = s * ok
            c = c * ok
        obj_real[row : row + SUBS, :] = c
        obj_imag[row : row + SUBS, :] = s

    for r in range(0, rows, SUBS):
        part = slice(r, r + SUBS)
        put(2 * rows + r, own[part, :], None)
        put(rows + r, jnp.where(is_second, mate[part, :], relay[part, :]), 3)
        put(3 * rows + r, jnp.where(is_second, relay[part, :], mate[part, :]), 4)
        if r >= rows - far:
            put(r, jnp.where(is_lower, pair[part, :], next_pair[part, :]), 2)
        if r < far:
            put(4 * rows + r, jnp.where(is_lower, next_pair[part, :], pair[part, :]), 5)

    lane = lax.broadcasted_iota(jnp.int32, (SUBS, LANES), 1)
    sub = lax.broadcasted_iota(jnp.int32, (SUBS, LANES), 0)

    def first_row(p):
        return ROWS_DEV // 4 + jitter[0, p]

    def masks(p):
        _, corner = window_place(p, patch)
        after = lane >= corner + jitter[1, p]
        below = [sub + k * SUBS >= first_row(p) for k in range(near // SUBS)]
        return after, below

    def pick(ref, p, k, after, below):
        tile, _ = window_place(p, patch)

        def at(row):
            left = ref[row : row + SUBS, tile * LANES : (tile + 1) * LANES] if tile >= 0 else 0.0
            right = (
                ref[row : row + SUBS, (tile + 1) * LANES : (tile + 2) * LANES]
                if tile + 1 < tiles
                else 0.0
            )
            return jnp.where(after, left, right)

        row = k * SUBS
        if row + SUBS <= ROWS_DEV // 4:
            return at(row + patch)
        if row < near:
            return jnp.where(below[k], at(row), at(row + patch))
        return at(row)

    def against(high, low, t_high, t_low):
        return dot(jnp.concatenate([high, low, high], 1), jnp.concatenate([t_high, t_high, t_low], 0))

    def onto(t_high, t_low, high, low):
        return dot(jnp.concatenate([t_high, t_high, t_low], 1), jnp.concatenate([high, low, high], 0))

    steps = patch // SUBS
    for p in range(number):
        after, below = masks(p)
        _, corner = window_place(p, patch)
        shift = corner + jitter[1, p]
        start = patch - first_row(p)
        p_real = pltpu.roll(twice[0, pl.ds(start, patch), :], shift, 1)
        p_imag = pltpu.roll(twice[1, pl.ds(start, patch), :], shift, 1)
        for k in range(steps):
            o_real = pick(obj_real, p, k, after, below)
            o_imag = pick(obj_imag, p, k, after, below)
            a = p_real[k * SUBS : (k + 1) * SUBS]
            b = p_imag[k * SUBS : (k + 1) * SUBS]
            row = p * patch + k * SUBS
            wave[row : row + SUBS, :LANES] = a * o_real - b * o_imag
            wave[row : row + SUBS, LANES:] = a * o_imag + b * o_real

    for p in range(0, number, 2):
        high, low = parts_of(wave[p * patch : (p + 2) * patch, :])
        mid[p * patch : (p + 2) * patch, :] = against(high, low, fwd_high, fwd_low)

    def upright(value):
        top = jnp.concatenate([value[:patch, :LANES], value[patch:, :LANES]], 1)
        low = jnp.concatenate([value[:patch, LANES:], value[patch:, LANES:]], 1)
        return jnp.concatenate([top, low], 0)

    total = jnp.zeros((SUBS, LANES), jnp.float32)
    for p in range(0, number, 2):
        high, low = parts_of(upright(mid[p * patch : (p + 2) * patch, :]))
        spectrum = onto(inv_high, inv_low, high, low)
        real, imag = spectrum[:patch], spectrum[patch:]
        target = jnp.concatenate([measured[p], measured[p + 1]], 1).astype(jnp.float32)
        power = real * real + imag * imag
        inverse = lax.rsqrt(jnp.maximum(power, 1e-30))
        error = power * inverse - target
        square = error * error
        for k in range(steps):
            for half in range(2):
                total += square[k * SUBS : (k + 1) * SUBS, half * LANES : (half + 1) * LANES]
        ratio = target * jnp.minimum(inverse, FLOOR_RATIO)
        high, low = parts_of(jnp.concatenate([ratio * real, ratio * imag], 0))
        undone = onto(fwd_high, fwd_low, high, low)
        for half in range(2):
            row = (p + half) * patch
            lanes = slice(half * LANES, (half + 1) * LANES)
            back[row : row + patch, :LANES] = undone[:patch, lanes]
            back[row : row + patch, LANES:] = undone[patch:, lanes]
    to_mate[2 * rows : 2 * rows + SUBS, :] = jnp.zeros((SUBS, cols), jnp.float32)
    to_mate[2 * rows : 2 * rows + SUBS, :LANES] = total

    for p in range(0, number, 2):
        high, low = parts_of(back[p * patch : (p + 2) * patch, :])
        out = against(high, low, inv_high, inv_low)
        w = wave[p * patch : (p + 2) * patch, :]
        mid[p * patch : (p + 2) * patch, :LANES] = w[:, :LANES] * out[:, LANES:] - w[:, LANES:] * out[:, :LANES]

    for t in range(tiles):
        meets = []
        for p in range(number):
            tile, _ = window_place(p, patch)
            if t in (tile, tile + 1):
                after, below = masks(p)
                meets.append((p, after if t == tile else jnp.logical_not(after), below))
        cols = slice(t * LANES, (t + 1) * LANES)
        for k in range(steps):
            row = k * SUBS
            here = there = None
            for p, mask, below in meets:
                term = jnp.where(mask, mid[p * patch + row : p * patch + row + SUBS, :LANES], 0.0)
                if row + SUBS <= ROWS_DEV // 4:
                    there = term if there is None else there + term
                elif row < near:
                    kept = jnp.where(below[k], term, 0.0)
                    here = kept if here is None else here + kept
                    there = (term - kept) if there is None else there + (term - kept)
                else:
                    here = term if here is None else here + term
            if here is not None:
                grad[row : row + SUBS, cols] = here
            else:
                grad[row : row + SUBS, cols] = jnp.zeros((SUBS, LANES), jnp.float32)
            if there is not None:
                grad[row + patch : row + patch + SUBS, cols] = there
    for row in range(patch + near, 5 * rows, SUBS):
        grad[row : row + SUBS, :] = jnp.zeros((SUBS, grad.shape[1]), jnp.float32)


    for r in range(0, rows, SUBS):
        part = slice(r, r + SUBS)
        up2, up1, here, dn1, dn2 = (grad[k * rows + r : k * rows + r + SUBS, :] for k in range(5))
        mine[part, :] = here
        to_mate[part, :] = jnp.where(is_second, up1, dn1)
        to_mate[rows + r : rows + r + SUBS, :] = jnp.where(is_second, dn1, up1)
        by_pair[part, :] = jnp.where(is_lower, up2, dn2)
        by_next[part, :] = jnp.where(is_lower, dn2, up2)


def strip_gradient(scalars, own, mate, pair, next_pair, relay, probe, measured):
    number, patch, _ = measured.shape
    rows, cols = own.shape
    vmem = pl.BlockSpec(memory_space=pltpu.VMEM)
    smem = pl.BlockSpec(memory_space=pltpu.SMEM)
    f32 = jnp.float32
    row = jax.ShapeDtypeStruct((rows, cols), f32)
    return pl.pallas_call(
        strip_kernel,
        out_shape=(row, jax.ShapeDtypeStruct((2 * rows + SUBS, cols), f32), row, row),
        in_specs=[smem] + [vmem] * 8,
        out_specs=(vmem,) * 4,
        scratch_shapes=[
            pltpu.VMEM((5 * rows, cols), f32),
            pltpu.VMEM((5 * rows, cols), f32),
            pltpu.VMEM((5 * rows, cols), f32),
            pltpu.VMEM((number * patch, 2 * LANES), f32),
            pltpu.VMEM((2, 2 * patch, patch), f32),
            pltpu.VMEM((number * patch, 2 * LANES), f32),
            pltpu.VMEM((number * patch, 2 * LANES), f32),
        ],
        compiler_params=pltpu.CompilerParams(vmem_limit_bytes=40 * 1024 * 1024),
        cost_estimate=pl.CostEstimate(
            flops=24 * number * patch**3 * 4, bytes_accessed=4 * number * patch * patch, transcendentals=0
        ),
        name="strip",
    )(scalars, own, mate, pair, next_pair, relay, probe, measured, dft_tables(patch))


def permuted(value, axis, target):
    count = lax.axis_size(axis)
    pairs = [(i, target(i)) for i in range(count) if 0 <= target(i) < count]
    return lax.ppermute(value, axis, pairs)


def with_mate(value):
    return permuted(value, "wide", lambda i: i ^ 1)


def with_pair(value):
    return permuted(value, "wide", lambda i: i ^ 2)


def to_next(value, back=False):
    return permuted(value, "wide", lambda i: i + 4 if (i // 2 % 2 == 0) != back else i - 4)


def joined(value, axis, steps):
    for step in steps:
        value = value + permuted(value, axis, lambda i: i ^ step)
    return value


def body(volume, path_lengths, probe, measured, jitter, step_sizes):
    groups = lax.axis_size("blk")
    column = lax.axis_index("wide")
    columns = lax.axis_size("wide")
    slab = volume[0]
    rows = slab.shape[1]

    def to_group(value, step):
        return lax.ppermute(value, "blk", [(i, (i + step) % groups) for i in range(groups)])

    terms, factors, scalars = slab_terms(slab, path_lengths, jitter[:, 0, 0], step_sizes, groups)
    own = terms[0]
    for step in range(1, groups):
        own = own + to_group(terms[step], step)

    even = column % 2 == column // 2 % 2
    pair = with_pair(own)
    mate = with_mate(own)
    next_pair = to_next(pair)
    relay = with_mate(jnp.where(even, pair, next_pair))
    mine, to_mate, by_pair, by_next = strip_gradient(
        scalars, own, mate, pair, next_pair, relay, probe, measured[0, 0]
    )
    got = with_mate(to_mate)
    mine = mine + got[:rows]
    passed = got[rows : 2 * rows]
    local = to_mate[2 * rows :, :LANES] + got[2 * rows :, :LANES]
    zero = jnp.zeros_like(passed)
    arrived = to_next(by_next + jnp.where(even, zero, passed), back=True)
    local = joined(local, "wide", [4])
    arrived, local = lax.optimization_barrier((arrived, local))
    gradient = mine + with_pair(by_pair + jnp.where(even, passed, zero) + arrived)
    others = [2**k for k in range(1, columns.bit_length() - 1) if k != 2]
    local = joined(local, "wide", others[1:])
    gradient, local = lax.optimization_barrier((gradient, local))
    grads = [gradient] + [to_group(gradient, step) for step in range(1, groups)]
    local = joined(local, "wide", others[:1])
    local = joined(local, "blk", [2**k for k in range(groups.bit_length() - 1)])
    return (updated(slab, factors, grads)[None], jnp.sum(local))


def solution(mesh):
    in_specs = (
        P("blk", None, "wide", None),
        P(),
        P(),
        P("blk", "wide", None, None, None),
        P(None, "blk", "wide", None),
        P(),
    )
    out_specs = (P("blk", None, "wide", None), P())
    return jax.shard_map(body, mesh=mesh, in_specs=in_specs, out_specs=out_specs, check_vma=False)
```

```python
import functools
import math

import jax
import jax.numpy as jnp
import numpy as np
from jax import lax
from jax.experimental import pallas as pl
from jax.experimental.pallas import tpu as pltpu
from jax.sharding import PartitionSpec as P

ROWS_DEV = 32
CSTEP = 64
JIT = 16
FLOOR_RATIO = 4.0
LANES = 128
SUBS = 8
HALF_PI = (1.5703125, 4.837512969970703125e-4, 7.54978995489188216e-8)


def dft_tables(length):
    grid = np.arange(length)
    angles = (grid[:, None] * grid[None, :] % length) * (2.0 * math.pi / length)
    cos = np.cos(angles) / math.sqrt(length)
    sin = -np.sin(angles) / math.sqrt(length)
    table = np.block([[cos, sin], [-sin, cos]])
    high = table.astype(jnp.bfloat16)
    low = (table - high.astype(np.float64)).astype(jnp.bfloat16)
    return np.stack([high, low, high.T, low.T])


def sin_cos(x):
    turns = jnp.floor(x * (2.0 / math.pi) + 0.5)
    r = x - turns * HALF_PI[0]
    r = r - turns * HALF_PI[1]
    r = r - turns * HALF_PI[2]
    quadrant = turns.astype(jnp.int32)
    z = r * r
    s = r + r * z * (-1.6666654611e-1 + z * (8.3321608736e-3 + z * -1.9515295891e-4))
    c = 1.0 - 0.5 * z + z * z * (
        4.166664568298827e-2 + z * (-1.388731625493765e-3 + z * 2.443315711809948e-5)
    )
    odd = (quadrant & 1) == 1
    sin = jnp.where(odd, c, s)
    cos = jnp.where(odd, s, c)
    sin = jnp.where((quadrant & 2) == 2, -sin, sin)
    cos = jnp.where(((quadrant + 1) & 2) == 2, -cos, cos)
    return sin, cos


def parts_of(x):
    high = x.astype(jnp.bfloat16)
    low = (x - high.astype(jnp.float32)).astype(jnp.bfloat16)
    return high, low


def window_place(position, patch):
    corner = patch // 4 - ROWS_DEV // 4 - patch // 2 + CSTEP * position
    tile = corner // LANES
    return tile, corner - tile * LANES


def term_of(slab, paths, angle, group, row):
    part = slab[0, row : row + SUBS, :] * paths[angle, group, 0]
    for layer in range(1, slab.shape[0]):
        part = part + slab[layer, row : row + SUBS, :] * paths[angle, group, layer]
    return part


def terms_kernel(slab_hbm, paths_hbm, *refs):
    terms = refs[:-3]
    slab, paths, sems = refs[-3:]
    groups = len(terms) + 1
    group = lax.axis_index("blk")
    copies = [
        pltpu.make_async_copy(slab_hbm, slab, sems.at[0]),
        pltpu.make_async_copy(paths_hbm, paths, sems.at[1]),
    ]
    for copy in copies:
        copy.start()
    for copy in copies:
        copy.wait()
    for step, term in enumerate(terms):
        angle = lax.rem(group + step + 1, groups)
        for r in range(0, slab.shape[1], SUBS):
            term[r : r + SUBS, :] = term_of(slab, paths, angle, group, r)


def slab_terms(slab, paths, groups):
    _, rows, cols = slab.shape
    f32 = jnp.float32
    return pl.pallas_call(
        terms_kernel,
        out_shape=[jax.ShapeDtypeStruct((rows, cols), f32)] * (groups - 1),
        in_specs=[pl.BlockSpec(memory_space=pltpu.HBM)] * 2,
        out_specs=[pl.BlockSpec(memory_space=pltpu.VMEM)] * (groups - 1),
        scratch_shapes=[
            pltpu.VMEM(slab.shape, f32),
            pltpu.SMEM(paths.shape, f32),
            pltpu.SemaphoreType.DMA((2,)),
        ],
        name="terms",
    )(slab, paths)


def own_kernel(groups, slab, paths, jitter, steps, term, factors, scalars):
    group = lax.axis_index("blk")
    column = lax.axis_index("wide")
    columns = lax.axis_size("wide")
    layers, rows, _ = slab.shape
    for p in range(jitter.shape[1]):
        scalars[0, p] = jitter[0, p]
        scalars[1, p] = jitter[1, p]
        scalars[2, p] = 0
    scalars[2, 0] = lax.rem(column, 2)
    scalars[2, 1] = lax.rem(column // 2, 2)
    scalars[2, 2] = (column >= 2).astype(jnp.int32)
    scalars[2, 3] = (column >= 1).astype(jnp.int32)
    scalars[2, 4] = (column + 1 < columns).astype(jnp.int32)
    scalars[2, 5] = (column + 2 < columns).astype(jnp.int32)
    for step in range(groups):
        source = lax.rem(group - step + groups, groups)
        for layer in range(layers):
            factors[step, layer] = jnp.full((SUBS, LANES), steps[source] * paths[source, group, layer], jnp.float32)
    for r in range(0, rows, SUBS):
        term[r : r + SUBS, :] = term_of(slab, paths, group, group, r)


def own_term(slab, paths, jitter, steps, groups):
    layers, rows, cols = slab.shape
    vmem = pl.BlockSpec(memory_space=pltpu.VMEM)
    smem = pl.BlockSpec(memory_space=pltpu.SMEM)
    f32 = jnp.float32
    return pl.pallas_call(
        functools.partial(own_kernel, groups),
        out_shape=(
            jax.ShapeDtypeStruct((rows, cols), f32),
            jax.ShapeDtypeStruct((groups, layers, SUBS, LANES), f32),
            jax.ShapeDtypeStruct((3, jitter.shape[1]), jnp.int32),
        ),
        in_specs=[vmem, smem, smem, smem],
        out_specs=(vmem, vmem, smem),
        compiler_params=pltpu.CompilerParams(vmem_limit_bytes=8 * 1024 * 1024),
        cost_estimate=pl.CostEstimate(flops=2**24, bytes_accessed=2**20, transcendentals=0),
        name="own",
    )(slab, paths, jitter, steps)


def update_kernel(slab, factors, *refs):
    grads, out = refs[:-1], refs[-1]
    layers, rows, cols = slab.shape
    for layer in range(layers):
        for r in range(0, rows, SUBS):
            for c in range(0, cols, LANES):
                value = slab[layer, r : r + SUBS, c : c + LANES]
                for step, grad in enumerate(grads):
                    value = value - factors[step, layer] * grad[r : r + SUBS, c : c + LANES]
                out[layer, r : r + SUBS, c : c + LANES] = value


def prepare_kernel(number, scalars, probe, tables, rolled, kept, twice):
    patch = probe.shape[1]
    for half in range(2):
        for part in range(2):
            twice[part, half * patch : (half + 1) * patch, :] = probe[part]
    for p in range(number):
        _, corner = window_place(p, patch)
        shift = corner + scalars[1, p]
        start = patch - ROWS_DEV // 4 - scalars[0, p]
        for part in range(2):
            value = pltpu.roll(twice[part, pl.ds(start, patch), :], shift, 1)
            rolled[p * patch : (p + 1) * patch, part * LANES : (part + 1) * LANES] = value
    for i in range(tables.shape[0]):
        kept[i] = tables[i]


def prepared(scalars, probe):
    number, patch = scalars.shape[1], probe.shape[1]
    tables = dft_tables(patch)
    vmem = pl.BlockSpec(memory_space=pltpu.VMEM)
    return pl.pallas_call(
        functools.partial(prepare_kernel, number),
        out_shape=(
            jax.ShapeDtypeStruct((number * patch, 2 * LANES), jnp.float32),
            jax.ShapeDtypeStruct(tables.shape, tables.dtype),
        ),
        in_specs=[pl.BlockSpec(memory_space=pltpu.SMEM), vmem, vmem],
        out_specs=(vmem, vmem),
        scratch_shapes=[pltpu.VMEM((2, 2 * patch, patch), jnp.float32)],
        compiler_params=pltpu.CompilerParams(vmem_limit_bytes=16 * 1024 * 1024),
        cost_estimate=pl.CostEstimate(flops=2**27, bytes_accessed=2**22, transcendentals=0),
        name="prepare",
    )(scalars, probe, tables)


def updated(slab, factors, grads):
    vmem = pl.BlockSpec(memory_space=pltpu.VMEM)
    return pl.pallas_call(
        update_kernel,
        out_shape=jax.ShapeDtypeStruct(slab.shape, slab.dtype),
        in_specs=[vmem] * (2 + len(grads)),
        out_specs=vmem,
        compiler_params=pltpu.CompilerParams(vmem_limit_bytes=8 * 1024 * 1024),
        name="update",
    )(slab, factors, *grads)


def strip_kernel(
    scalars,
    own,
    mate,
    pair,
    next_pair,
    relay,
    rolled,
    measured,
    tables,
    mine,
    to_mate,
    by_pair,
    by_next,
    obj_real,
    obj_imag,
    grad,
    wave,
    mid,
    back,
):
    number, patch, _ = measured.shape
    rows, cols = own.shape
    tiles = cols // LANES
    far = rows - ROWS_DEV // 4
    near = ROWS_DEV // 4 + JIT
    dot = functools.partial(lax.dot, preferred_element_type=jnp.float32)
    jitter = scalars

    def flag(index):
        return jnp.full((SUBS, cols), scalars[2, index], jnp.int32) == 1

    is_second = flag(0)
    is_lower = flag(1)
    fwd_high, fwd_low, inv_high, inv_low = (tables[i] for i in range(4))

    def put(row, phase, index):
        s, c = sin_cos(phase)
        if index is not None:
            ok = scalars[2, index].astype(jnp.float32)
            s = s * ok
            c = c * ok
        obj_real[row : row + SUBS, :] = c
        obj_imag[row : row + SUBS, :] = s

    for r in range(0, rows, SUBS):
        part = slice(r, r + SUBS)
        put(2 * rows + r, own[part, :], None)
        put(rows + r, jnp.where(is_second, mate[part, :], relay[part, :]), 3)
        put(3 * rows + r, jnp.where(is_second, relay[part, :], mate[part, :]), 4)
        if r >= rows - far:
            put(r, jnp.where(is_lower, pair[part, :], next_pair[part, :]), 2)
        if r < far:
            put(4 * rows + r, jnp.where(is_lower, next_pair[part, :], pair[part, :]), 5)

    lane = lax.broadcasted_iota(jnp.int32, (SUBS, LANES), 1)
    sub = lax.broadcasted_iota(jnp.int32, (SUBS, LANES), 0)

    def first_row(p):
        return ROWS_DEV // 4 + jitter[0, p]

    def masks(p):
        _, corner = window_place(p, patch)
        after = lane >= corner + jitter[1, p]
        below = [sub + k * SUBS >= first_row(p) for k in range(near // SUBS)]
        return after, below

    def pick(ref, p, k, after, below):
        tile, _ = window_place(p, patch)

        def at(row):
            left = ref[row : row + SUBS, tile * LANES : (tile + 1) * LANES] if tile >= 0 else 0.0
            right = (
                ref[row : row + SUBS, (tile + 1) * LANES : (tile + 2) * LANES]
                if tile + 1 < tiles
                else 0.0
            )
            return jnp.where(after, left, right)

        row = k * SUBS
        if row + SUBS <= ROWS_DEV // 4:
            return at(row + patch)
        if row < near:
            return jnp.where(below[k], at(row), at(row + patch))
        return at(row)

    def against(high, low, t_high, t_low):
        return dot(jnp.concatenate([high, low, high], 1), jnp.concatenate([t_high, t_high, t_low], 0))

    def onto(t_high, t_low, high, low):
        return dot(jnp.concatenate([t_high, t_high, t_low], 1), jnp.concatenate([high, low, high], 0))

    steps = patch // SUBS
    for p in range(number):
        after, below = masks(p)
        for k in range(steps):
            o_real = pick(obj_real, p, k, after, below)
            o_imag = pick(obj_imag, p, k, after, below)
            row = p * patch + k * SUBS
            a = rolled[row : row + SUBS, :LANES]
            b = rolled[row : row + SUBS, LANES:]
            wave[row : row + SUBS, :LANES] = a * o_real - b * o_imag
            wave[row : row + SUBS, LANES:] = a * o_imag + b * o_real

    for p in range(0, number, 2):
        high, low = parts_of(wave[p * patch : (p + 2) * patch, :])
        mid[p * patch : (p + 2) * patch, :] = against(high, low, fwd_high, fwd_low)

    def upright(value):
        top = jnp.concatenate([value[:patch, :LANES], value[patch:, :LANES]], 1)
        low = jnp.concatenate([value[:patch, LANES:], value[patch:, LANES:]], 1)
        return jnp.concatenate([top, low], 0)

    total = jnp.zeros((SUBS, LANES), jnp.float32)
    for p in range(0, number, 2):
        high, low = parts_of(upright(mid[p * patch : (p + 2) * patch, :]))
        spectrum = onto(inv_high, inv_low, high, low)
        real, imag = spectrum[:patch], spectrum[patch:]
        target = jnp.concatenate([measured[p], measured[p + 1]], 1).astype(jnp.float32)
        power = real * real + imag * imag
        inverse = lax.rsqrt(jnp.maximum(power, 1e-30))
        error = power * inverse - target
        square = error * error
        for k in range(steps):
            for half in range(2):
                total += square[k * SUBS : (k + 1) * SUBS, half * LANES : (half + 1) * LANES]
        ratio = target * jnp.minimum(inverse, FLOOR_RATIO)
        high, low = parts_of(jnp.concatenate([ratio * real, ratio * imag], 0))
        undone = onto(fwd_high, fwd_low, high, low)
        for half in range(2):
            row = (p + half) * patch
            lanes = slice(half * LANES, (half + 1) * LANES)
            back[row : row + patch, :LANES] = undone[:patch, lanes]
            back[row : row + patch, LANES:] = undone[patch:, lanes]
    to_mate[2 * rows : 2 * rows + SUBS, :] = jnp.zeros((SUBS, cols), jnp.float32)
    to_mate[2 * rows : 2 * rows + SUBS, :LANES] = total

    for p in range(0, number, 2):
        high, low = parts_of(back[p * patch : (p + 2) * patch, :])
        out = against(high, low, inv_high, inv_low)
        w = wave[p * patch : (p + 2) * patch, :]
        mid[p * patch : (p + 2) * patch, :LANES] = w[:, :LANES] * out[:, LANES:] - w[:, LANES:] * out[:, :LANES]

    for t in range(tiles):
        meets = []
        for p in range(number):
            tile, _ = window_place(p, patch)
            if t in (tile, tile + 1):
                after, below = masks(p)
                meets.append((p, after if t == tile else jnp.logical_not(after), below))
        cols = slice(t * LANES, (t + 1) * LANES)
        for k in range(steps):
            row = k * SUBS
            here = there = None
            for p, mask, below in meets:
                term = jnp.where(mask, mid[p * patch + row : p * patch + row + SUBS, :LANES], 0.0)
                if row + SUBS <= ROWS_DEV // 4:
                    there = term if there is None else there + term
                elif row < near:
                    kept = jnp.where(below[k], term, 0.0)
                    here = kept if here is None else here + kept
                    there = (term - kept) if there is None else there + (term - kept)
                else:
                    here = term if here is None else here + term
            if here is not None:
                grad[row : row + SUBS, cols] = here
            else:
                grad[row : row + SUBS, cols] = jnp.zeros((SUBS, LANES), jnp.float32)
            if there is not None:
                grad[row + patch : row + patch + SUBS, cols] = there
    for row in range(patch + near, 5 * rows, SUBS):
        grad[row : row + SUBS, :] = jnp.zeros((SUBS, grad.shape[1]), jnp.float32)


    for r in range(0, rows, SUBS):
        part = slice(r, r + SUBS)
        up2, up1, here, dn1, dn2 = (grad[k * rows + r : k * rows + r + SUBS, :] for k in range(5))
        mine[part, :] = here
        to_mate[part, :] = jnp.where(is_second, up1, dn1)
        to_mate[rows + r : rows + r + SUBS, :] = jnp.where(is_second, dn1, up1)
        by_pair[part, :] = jnp.where(is_lower, up2, dn2)
        by_next[part, :] = jnp.where(is_lower, dn2, up2)


def strip_gradient(scalars, own, mate, pair, next_pair, relay, rolled, measured, tables):
    number, patch, _ = measured.shape
    rows, cols = own.shape
    vmem = pl.BlockSpec(memory_space=pltpu.VMEM)
    smem = pl.BlockSpec(memory_space=pltpu.SMEM)
    f32 = jnp.float32
    row = jax.ShapeDtypeStruct((rows, cols), f32)
    return pl.pallas_call(
        strip_kernel,
        out_shape=(row, jax.ShapeDtypeStruct((2 * rows + SUBS, cols), f32), row, row),
        in_specs=[smem] + [vmem] * 8,
        out_specs=(vmem,) * 4,
        scratch_shapes=[
            pltpu.VMEM((5 * rows, cols), f32),
            pltpu.VMEM((5 * rows, cols), f32),
            pltpu.VMEM((5 * rows, cols), f32),
            pltpu.VMEM((number * patch, 2 * LANES), f32),
            pltpu.VMEM((number * patch, 2 * LANES), f32),
            pltpu.VMEM((number * patch, 2 * LANES), f32),
        ],
        compiler_params=pltpu.CompilerParams(vmem_limit_bytes=40 * 1024 * 1024),
        cost_estimate=pl.CostEstimate(
            flops=24 * number * patch**3 * 4, bytes_accessed=4 * number * patch * patch, transcendentals=0
        ),
        name="strip",
    )(scalars, own, mate, pair, next_pair, relay, rolled, measured, tables)


def permuted(value, axis, target):
    count = lax.axis_size(axis)
    pairs = [(i, target(i)) for i in range(count) if 0 <= target(i) < count]
    return lax.ppermute(value, axis, pairs)


def with_mate(value):
    return permuted(value, "wide", lambda i: i ^ 1)


def with_pair(value):
    return permuted(value, "wide", lambda i: i ^ 2)


def across(value):
    count = lax.axis_size("wide")

    def target(i):
        j = i + 2 if i // 2 % 2 else i - 2
        return j if 0 <= j < count else i ^ 1

    return permuted(value, "wide", target)


def joined(value, axis, steps):
    for step in steps:
        value = value + permuted(value, axis, lambda i: i ^ step)
    return value


def program(volume, path_lengths, probe, measured, jitter, step_sizes):
    groups = lax.axis_size("blk")
    column = lax.axis_index("wide")
    columns = lax.axis_size("wide")
    slab = volume[0]
    rows = slab.shape[1]

    def to_group(value, step):
        return lax.ppermute(value, "blk", [(i, (i + step) % groups) for i in range(groups)])

    terms = slab_terms(slab, path_lengths, groups)
    own, factors, scalars = own_term(slab, path_lengths, jitter[:, 0, 0], step_sizes, groups)
    for step in range(1, groups):
        own = own + to_group(terms[step - 1], step)

    even = column % 2 == column // 2 % 2
    next_pair = across(own)
    pair = with_pair(own)
    rolled, tables = prepared(scalars, probe)
    both = with_mate(jnp.concatenate([own, jnp.where(even, pair, next_pair)], 0))
    mate, relay = both[:rows], both[rows:]
    mine, to_mate, by_pair, by_next = strip_gradient(
        scalars, own, mate, pair, next_pair, relay, rolled, measured[0, 0], tables
    )
    got = with_mate(to_mate)
    mine = mine + got[:rows]
    passed = got[rows : 2 * rows]
    local = to_mate[2 * rows :, :LANES] + got[2 * rows :, :LANES]
    zero = jnp.zeros_like(passed)
    from_next = across(by_next + jnp.where(even, zero, passed))
    from_pair = with_pair(by_pair + jnp.where(even, passed, zero))
    local = joined(local, "blk", [2**k for k in range(groups.bit_length() - 1)])
    wide_steps = [2**k for k in range(2, columns.bit_length() - 1)]
    local = joined(local, "wide", wide_steps[:1])
    from_next, from_pair, local = lax.optimization_barrier((from_next, from_pair, local))
    gradient = mine + from_next + from_pair
    grads = [gradient]
    for step in range(1, groups):
        grads.append(to_group(gradient, step))
    local = joined(local, "wide", ([2] + wide_steps[1:])[:-1])
    local = joined(local, "wide", ([2] + wide_steps[1:])[-1:])
    new = updated(slab, factors, grads)
    return (new[None], jnp.sum(local))


def solution(mesh):
    in_specs = (
        P("blk", None, "wide", None),
        P(),
        P(),
        P("blk", "wide", None, None, None),
        P(None, "blk", "wide", None),
        P(),
    )
    out_specs = (P("blk", None, "wide", None), P())
    return jax.shard_map(program, mesh=mesh, in_specs=in_specs, out_specs=out_specs, check_vma=False)
```

```python
import functools
import math

import jax
import jax.numpy as jnp
import numpy as np
from jax import lax
from jax.experimental import pallas as pl
from jax.experimental.pallas import tpu as pltpu
from jax.sharding import PartitionSpec as P

ROWS_DEV = 32
CSTEP = 64
JIT = 16
FLOOR_RATIO = 4.0
LANES = 128
SUBS = 8
HALF_PI = (1.5703125, 4.837512969970703125e-4, 7.54978995489188216e-8)


def dft_tables(length):
    grid = np.arange(length)
    angles = (grid[:, None] * grid[None, :] % length) * (2.0 * math.pi / length)
    cos = np.cos(angles) / math.sqrt(length)
    sin = -np.sin(angles) / math.sqrt(length)
    table = np.block([[cos, sin], [-sin, cos]])
    high = table.astype(jnp.bfloat16)
    low = (table - high.astype(np.float64)).astype(jnp.bfloat16)
    return np.stack([high, low, high.T, low.T])


def sin_cos(x):
    turns = jnp.floor(x * (2.0 / math.pi) + 0.5)
    r = x - turns * HALF_PI[0]
    r = r - turns * HALF_PI[1]
    r = r - turns * HALF_PI[2]
    quadrant = turns.astype(jnp.int32)
    z = r * r
    s = r + r * z * (-1.6666654611e-1 + z * (8.3321608736e-3 + z * -1.9515295891e-4))
    c = 1.0 - 0.5 * z + z * z * (
        4.166664568298827e-2 + z * (-1.388731625493765e-3 + z * 2.443315711809948e-5)
    )
    odd = (quadrant & 1) == 1
    sin = jnp.where(odd, c, s)
    cos = jnp.where(odd, s, c)
    sin = jnp.where((quadrant & 2) == 2, -sin, sin)
    cos = jnp.where(((quadrant + 1) & 2) == 2, -cos, cos)
    return sin, cos


def parts_of(x):
    high = x.astype(jnp.bfloat16)
    low = (x - high.astype(jnp.float32)).astype(jnp.bfloat16)
    return high, low


def window_place(position, patch):
    corner = patch // 4 - ROWS_DEV // 4 - patch // 2 + CSTEP * position
    tile = corner // LANES
    return tile, corner - tile * LANES


def term_of(slab, paths, angle, group, row, col):
    part = slab[0, row : row + SUBS, col : col + LANES] * paths[angle, group, 0]
    for layer in range(1, slab.shape[0]):
        part = part + slab[layer, row : row + SUBS, col : col + LANES] * paths[angle, group, layer]
    return part


def blocks_of(rows, cols):
    wide = cols // LANES
    return [(r // SUBS * wide + c // LANES, r, c) for r in range(0, rows, SUBS) for c in range(0, cols, LANES)]


def terms_kernel(groups, slab_hbm, paths_hbm, jitter_hbm, steps_hbm, *refs):
    terms, factors, scalars = refs[: groups - 1], refs[groups - 1], refs[groups]
    slab, paths, jitter, steps, sems = refs[groups + 1 :]
    group = lax.axis_index("blk")
    column = lax.axis_index("wide")
    columns = lax.axis_size("wide")
    sources = (slab_hbm, paths_hbm, jitter_hbm, steps_hbm)
    copies = [
        pltpu.make_async_copy(source, target, sems.at[i])
        for i, (source, target) in enumerate(zip(sources, (slab, paths, jitter, steps)))
    ]
    for copy in copies:
        copy.start()
    for copy in copies[1:]:
        copy.wait()
    for p in range(jitter.shape[1]):
        scalars[0, p] = jitter[0, p]
        scalars[1, p] = jitter[1, p]
        scalars[2, p] = 0
    scalars[2, 0] = lax.rem(column, 2)
    scalars[2, 1] = lax.rem(column // 2, 2)
    scalars[2, 2] = (column >= 2).astype(jnp.int32)
    scalars[2, 3] = (column >= 1).astype(jnp.int32)
    scalars[2, 4] = (column + 1 < columns).astype(jnp.int32)
    scalars[2, 5] = (column + 2 < columns).astype(jnp.int32)
    layers, rows, cols = slab.shape
    for step in range(groups):
        source = lax.rem(group - step + groups, groups)
        for layer in range(layers):
            factors[step, layer] = jnp.full((SUBS, LANES), steps[source] * paths[source, group, layer], jnp.float32)
    copies[0].wait()
    for step, term in enumerate(terms):
        angle = lax.rem(group + step + 1, groups)
        for i, r, c in blocks_of(rows, cols):
            term[i] = term_of(slab, paths, angle, group, r, c)


def listed(slab, extra=0):
    _, rows, cols = slab.shape
    return jax.ShapeDtypeStruct((rows // SUBS * (cols // LANES) + extra, SUBS, LANES), jnp.float32)


def slab_terms(slab, paths, jitter, steps, groups):
    vmem = pl.BlockSpec(memory_space=pltpu.VMEM)
    out = pl.pallas_call(
        functools.partial(terms_kernel, groups),
        out_shape=[listed(slab)] * (groups - 1)
        + [
            jax.ShapeDtypeStruct((groups, slab.shape[0], SUBS, LANES), jnp.float32),
            jax.ShapeDtypeStruct((3, jitter.shape[1]), jnp.int32),
        ],
        in_specs=[pl.BlockSpec(memory_space=pltpu.HBM)] * 4,
        out_specs=[vmem] * groups + [pl.BlockSpec(memory_space=pltpu.SMEM)],
        scratch_shapes=[
            pltpu.VMEM(slab.shape, jnp.float32),
            pltpu.SMEM(paths.shape, jnp.float32),
            pltpu.SMEM(jitter.shape, jnp.int32),
            pltpu.SMEM(steps.shape, jnp.float32),
            pltpu.SemaphoreType.DMA((4,)),
        ],
        name="terms",
    )(slab, paths, jitter, steps)
    return out[: groups - 1], out[groups - 1], out[groups]


def own_kernel(slab, paths, term):
    group = lax.axis_index("blk")
    for i, r, c in blocks_of(*slab.shape[1:]):
        term[i] = term_of(slab, paths, group, group, r, c)


def own_term(slab, paths):
    return pl.pallas_call(
        own_kernel,
        out_shape=listed(slab),
        in_specs=[pl.BlockSpec(memory_space=pltpu.VMEM), pl.BlockSpec(memory_space=pltpu.SMEM)],
        out_specs=pl.BlockSpec(memory_space=pltpu.VMEM),
        compiler_params=pltpu.CompilerParams(vmem_limit_bytes=8 * 1024 * 1024),
        cost_estimate=pl.CostEstimate(flops=2**24, bytes_accessed=2**20, transcendentals=0),
        name="own",
    )(slab, paths)


def update_kernel(count, slab, factors, *refs):
    grads, sums, out, total = refs[:count], refs[count:-2], refs[-2], refs[-1]
    layers, rows, cols = slab.shape
    blocks = grads[0].shape[0]
    value = sums[0][0]
    if len(sums) == 3:
        value = (value + sums[1][0]) + (grads[1][blocks] + sums[2][0])
    total[0, 0] = jnp.sum(value)
    for layer in range(layers):
        for i, r, c in blocks_of(rows, cols):
            value = slab[layer, r : r + SUBS, c : c + LANES]
            for step in range(count):
                value = value - factors[step, layer] * grads[step][i]
            out[layer, r : r + SUBS, c : c + LANES] = value


def updated(slab, factors, grads, sums):
    vmem = pl.BlockSpec(memory_space=pltpu.VMEM)
    return pl.pallas_call(
        functools.partial(update_kernel, len(grads)),
        out_shape=(jax.ShapeDtypeStruct(slab.shape, slab.dtype), jax.ShapeDtypeStruct((1, 1), jnp.float32)),
        in_specs=[vmem] * (2 + len(grads) + len(sums)),
        out_specs=(vmem, pl.BlockSpec(memory_space=pltpu.SMEM)),
        compiler_params=pltpu.CompilerParams(vmem_limit_bytes=8 * 1024 * 1024),
        name="update",
    )(slab, factors, *grads, *sums)


def prepare_kernel(number, scalars, probe, tables, rolled, kept, twice):
    patch = probe.shape[1]
    for half in range(2):
        for part in range(2):
            twice[part, half * patch : (half + 1) * patch, :] = probe[part]
    for p in range(number):
        _, corner = window_place(p, patch)
        shift = corner + scalars[1, p]
        start = patch - ROWS_DEV // 4 - scalars[0, p]
        for part in range(2):
            value = pltpu.roll(twice[part, pl.ds(start, patch), :], shift, 1)
            rolled[p * patch : (p + 1) * patch, part * LANES : (part + 1) * LANES] = value
    for i in range(tables.shape[0]):
        kept[i] = tables[i]


def prepared(scalars, probe):
    number, patch = scalars.shape[1], probe.shape[1]
    tables = dft_tables(patch)
    vmem = pl.BlockSpec(memory_space=pltpu.VMEM)
    return pl.pallas_call(
        functools.partial(prepare_kernel, number),
        out_shape=(
            jax.ShapeDtypeStruct((number * patch, 2 * LANES), jnp.float32),
            jax.ShapeDtypeStruct(tables.shape, tables.dtype),
        ),
        in_specs=[pl.BlockSpec(memory_space=pltpu.SMEM), vmem, vmem],
        out_specs=(vmem, vmem),
        scratch_shapes=[pltpu.VMEM((2, 2 * patch, patch), jnp.float32)],
        compiler_params=pltpu.CompilerParams(vmem_limit_bytes=16 * 1024 * 1024),
        cost_estimate=pl.CostEstimate(flops=2**27, bytes_accessed=2**22, transcendentals=0),
        name="prepare",
    )(scalars, probe, tables)


def strip_kernel(
    scalars,
    own,
    mate,
    pair,
    next_pair,
    relay,
    rolled,
    measured,
    tables,
    mine,
    to_mate,
    by_pair,
    by_next,
    misfit,
    obj_real,
    obj_imag,
    wave,
    mid,
    back,
):
    number, patch, _ = measured.shape
    rows = ROWS_DEV
    tiles = own.shape[0] * SUBS // rows
    far = rows - ROWS_DEV // 4
    near = ROWS_DEV // 4 + JIT
    dot = functools.partial(lax.dot, preferred_element_type=jnp.float32)
    jitter = scalars

    def flag(index):
        return jnp.full((SUBS, LANES), scalars[2, index], jnp.int32) == 1

    is_second = flag(0)
    is_lower = flag(1)
    fwd_high, fwd_low, inv_high, inv_low = (tables[i] for i in range(4))

    def put(row, tile, phase, index):
        s, c = sin_cos(phase)
        if index is not None:
            ok = scalars[2, index].astype(jnp.float32)
            s = s * ok
            c = c * ok
        obj_real[row // SUBS * tiles + tile] = c
        obj_imag[row // SUBS * tiles + tile] = s

    for i, r, c in blocks_of(rows, tiles * LANES):
        t = c // LANES
        put(2 * rows + r, t, own[i], None)
        put(rows + r, t, jnp.where(is_second, mate[i], relay[i]), 3)
        put(3 * rows + r, t, jnp.where(is_second, relay[i], mate[i]), 4)
        if r >= rows - far:
            put(r, t, jnp.where(is_lower, pair[i], next_pair[i]), 2)
        if r < far:
            put(4 * rows + r, t, jnp.where(is_lower, next_pair[i], pair[i]), 5)

    lane = lax.broadcasted_iota(jnp.int32, (SUBS, LANES), 1)
    sub = lax.broadcasted_iota(jnp.int32, (SUBS, LANES), 0)

    def first_row(p):
        return ROWS_DEV // 4 + jitter[0, p]

    def masks(p):
        _, corner = window_place(p, patch)
        after = lane >= corner + jitter[1, p]
        below = [sub + k * SUBS >= first_row(p) for k in range(near // SUBS)]
        return after, below

    def pick(ref, p, k, after, below):
        tile, _ = window_place(p, patch)

        def at(row):
            first = row // SUBS * tiles + tile
            left = ref[first] if tile >= 0 else 0.0
            right = ref[first + 1] if tile + 1 < tiles else 0.0
            return jnp.where(after, left, right)

        row = k * SUBS
        if row + SUBS <= ROWS_DEV // 4:
            return at(row + patch)
        if row < near:
            return jnp.where(below[k], at(row), at(row + patch))
        return at(row)

    def against(high, low, t_high, t_low):
        return dot(jnp.concatenate([high, low, high], 1), jnp.concatenate([t_high, t_high, t_low], 0))

    def onto(t_high, t_low, high, low):
        return dot(jnp.concatenate([t_high, t_high, t_low], 1), jnp.concatenate([high, low, high], 0))

    steps = patch // SUBS
    for p in range(number):
        after, below = masks(p)
        for k in range(steps):
            o_real = pick(obj_real, p, k, after, below)
            o_imag = pick(obj_imag, p, k, after, below)
            row = p * patch + k * SUBS
            a = rolled[row : row + SUBS, :LANES]
            b = rolled[row : row + SUBS, LANES:]
            wave[row : row + SUBS, :LANES] = a * o_real - b * o_imag
            wave[row : row + SUBS, LANES:] = a * o_imag + b * o_real

    for p in range(0, number, 2):
        high, low = parts_of(wave[p * patch : (p + 2) * patch, :])
        mid[p * patch : (p + 2) * patch, :] = against(high, low, fwd_high, fwd_low)

    def upright(value):
        top = jnp.concatenate([value[:patch, :LANES], value[patch:, :LANES]], 1)
        low = jnp.concatenate([value[:patch, LANES:], value[patch:, LANES:]], 1)
        return jnp.concatenate([top, low], 0)

    total = jnp.zeros((SUBS, LANES), jnp.float32)
    for p in range(0, number, 2):
        high, low = parts_of(upright(mid[p * patch : (p + 2) * patch, :]))
        spectrum = onto(inv_high, inv_low, high, low)
        real, imag = spectrum[:patch], spectrum[patch:]
        target = jnp.concatenate([measured[p], measured[p + 1]], 1).astype(jnp.float32)
        power = real * real + imag * imag
        inverse = lax.rsqrt(jnp.maximum(power, 1e-30))
        error = power * inverse - target
        square = error * error
        for k in range(steps):
            for half in range(2):
                total += square[k * SUBS : (k + 1) * SUBS, half * LANES : (half + 1) * LANES]
        ratio = target * jnp.minimum(inverse, FLOOR_RATIO)
        high, low = parts_of(jnp.concatenate([ratio * real, ratio * imag], 0))
        undone = onto(fwd_high, fwd_low, high, low)
        for half in range(2):
            row = (p + half) * patch
            lanes = slice(half * LANES, (half + 1) * LANES)
            back[row : row + patch, :LANES] = undone[:patch, lanes]
            back[row : row + patch, LANES:] = undone[patch:, lanes]
    misfit[0] = total

    for p in range(0, number, 2):
        high, low = parts_of(back[p * patch : (p + 2) * patch, :])
        out = against(high, low, inv_high, inv_low)
        w = wave[p * patch : (p + 2) * patch, :]
        mid[p * patch : (p + 2) * patch, :LANES] = w[:, :LANES] * out[:, LANES:] - w[:, LANES:] * out[:, :LANES]

    grads = {}
    for t in range(tiles):
        meets = []
        for p in range(number):
            tile, _ = window_place(p, patch)
            if t in (tile, tile + 1):
                after, below = masks(p)
                meets.append((p, after if t == tile else jnp.logical_not(after), below))
        for k in range(steps):
            row = k * SUBS
            here = there = None
            for p, mask, below in meets:
                term = jnp.where(mask, mid[p * patch + row : p * patch + row + SUBS, :LANES], 0.0)
                if row + SUBS <= ROWS_DEV // 4:
                    there = term if there is None else there + term
                elif row < near:
                    kept = jnp.where(below[k], term, 0.0)
                    here = kept if here is None else here + kept
                    there = (term - kept) if there is None else there + (term - kept)
                else:
                    here = term if here is None else here + term
            grads[k, t] = here
            grads[k + steps, t] = there

    def add_to(slot, r, t):
        value = grads.get((slot * (rows // SUBS) + r // SUBS, t))
        return jnp.zeros((SUBS, LANES), jnp.float32) if value is None else value

    for i, r, c in blocks_of(rows, tiles * LANES):
        up2, up1, here, dn1, dn2 = (add_to(slot, r, c // LANES) for slot in range(5))
        mine[i] = here
        to_mate[i] = jnp.where(is_second, up1, dn1)
        to_mate[own.shape[0] + i] = jnp.where(is_second, dn1, up1)
        by_pair[i] = jnp.where(is_lower, up2, dn2)
        by_next[i] = jnp.where(is_lower, dn2, up2)


def strip_gradient(scalars, own, mate, pair, next_pair, relay, rolled, measured, tables):
    number, patch, _ = measured.shape
    blocks = own.shape[0]
    vmem = pl.BlockSpec(memory_space=pltpu.VMEM)
    smem = pl.BlockSpec(memory_space=pltpu.SMEM)

    def block_list(count):
        return jax.ShapeDtypeStruct((count, SUBS, LANES), jnp.float32)

    return pl.pallas_call(
        strip_kernel,
        out_shape=tuple(block_list(n) for n in (blocks, 2 * blocks, blocks, blocks, 1)),
        in_specs=[smem] + [vmem] * 8,
        out_specs=(vmem,) * 5,
        scratch_shapes=[
            pltpu.VMEM((5 * blocks, SUBS, LANES), jnp.float32),
            pltpu.VMEM((5 * blocks, SUBS, LANES), jnp.float32),
            pltpu.VMEM((number * patch, 2 * LANES), jnp.float32),
            pltpu.VMEM((number * patch, 2 * LANES), jnp.float32),
            pltpu.VMEM((number * patch, 2 * LANES), jnp.float32),
        ],
        compiler_params=pltpu.CompilerParams(vmem_limit_bytes=40 * 1024 * 1024),
        cost_estimate=pl.CostEstimate(
            flops=24 * number * patch**3 * 4, bytes_accessed=4 * number * patch * patch, transcendentals=0
        ),
        name="strip",
    )(scalars, own, mate, pair, next_pair, relay, rolled, measured, tables)


def permuted(value, axis, target):
    count = lax.axis_size(axis)
    pairs = [(i, target(i)) for i in range(count) if 0 <= target(i) < count]
    return lax.ppermute(value, axis, pairs)


def with_mate(value):
    return permuted(value, "wide", lambda i: i ^ 1)


def with_pair(value):
    return permuted(value, "wide", lambda i: i ^ 2)


def across(value):
    count = lax.axis_size("wide")

    def target(i):
        j = i + 2 if i // 2 % 2 else i - 2
        return j if 0 <= j < count else i ^ 1

    return permuted(value, "wide", target)


def joined(value, axis, steps):
    for step in steps:
        value = value + permuted(value, axis, lambda i: i ^ step)
    return value


def program(volume, path_lengths, probe, measured, jitter, step_sizes):
    groups = lax.axis_size("blk")
    column = lax.axis_index("wide")
    columns = lax.axis_size("wide")
    slab = volume[0]

    def to_group(value, step):
        return lax.ppermute(value, "blk", [(i, (i + step) % groups) for i in range(groups)])

    terms, factors, scalars = slab_terms(slab, path_lengths, jitter[:, 0, 0], step_sizes, groups)
    own = own_term(slab, path_lengths)
    for step in range(1, groups):
        own = own + to_group(terms[step - 1], step)

    even = column % 2 == column // 2 % 2
    next_pair = across(own)
    pair = with_pair(own)
    rolled, tables = prepared(scalars, probe)
    both = with_mate(jnp.concatenate([own, jnp.where(even, pair, next_pair)], 0))
    blocks = own.shape[0]
    mate, relay = both[:blocks], both[blocks:]
    mine, to_mate, by_pair, by_next, local = strip_gradient(
        scalars, own, mate, pair, next_pair, relay, rolled, measured[0, 0], tables
    )
    got = with_mate(to_mate)
    if groups != 2:
        local = joined(local, "blk", [2**k for k in range(groups.bit_length() - 1)])
    local = joined(local, "wide", [4])
    mine = mine + got[:blocks]
    passed = got[blocks:]
    zero = jnp.zeros_like(passed)
    from_pair = with_pair(by_pair + jnp.where(even, passed, zero))
    from_next = across(by_next + jnp.where(even, zero, passed))
    local = joined(local, "wide", [1])
    local = joined(local, "wide", [2**k for k in range(3, columns.bit_length() - 1)])
    gradient = mine + (from_next + from_pair)
    grads = [gradient]
    if groups == 2:
        grads.append(to_group(jnp.concatenate([gradient, local], 0), 1))
        sums = [local, with_pair(local)]
        pairs = [(i, (i + columns) % (2 * columns) ^ 2) for i in range(2 * columns)]
        sums.append(lax.ppermute(local, ("blk", "wide"), pairs))
    else:
        for step in range(1, groups):
            grads.append(to_group(gradient, step))
        sums = [joined(local, "wide", [2])]
    new, total = updated(slab, factors, grads, sums)
    return (new[None], total[0, 0])


def solution(mesh):
    in_specs = (
        P("blk", None, "wide", None),
        P(),
        P(),
        P("blk", "wide", None, None, None),
        P(None, "blk", "wide", None),
        P(),
    )
    out_specs = (P("blk", None, "wide", None), P())
    return jax.shard_map(program, mesh=mesh, in_specs=in_specs, out_specs=out_specs, check_vma=False)
```

```python
import functools
import math

import jax
import jax.numpy as jnp
import numpy as np
from jax import lax
from jax.experimental import pallas as pl
from jax.experimental.pallas import tpu as pltpu
from jax.sharding import PartitionSpec as P

ROWS_DEV = 32
CSTEP = 64
JIT = 16
FLOOR_RATIO = 4.0
LANES = 128
TALL = 4
BROAD = 2
SUBS = 8
HALF_PI = (1.5703125, 4.837512969970703125e-4, 7.54978995489188216e-8)


def dft_tables(length):
    grid = np.arange(length)
    angles = (grid[:, None] * grid[None, :] % length) * (2.0 * math.pi / length)
    cos = np.cos(angles) / math.sqrt(length)
    sin = -np.sin(angles) / math.sqrt(length)
    table = np.block([[cos, sin], [-sin, cos]])
    high = table.astype(jnp.bfloat16)
    low = (table - high.astype(np.float64)).astype(jnp.bfloat16)
    return np.stack([high, low, high.T, low.T])


def sin_cos(x):
    turns = jnp.floor(x * (2.0 / math.pi) + 0.5)
    r = x - turns * HALF_PI[0]
    r = r - turns * HALF_PI[1]
    r = r - turns * HALF_PI[2]
    quadrant = turns.astype(jnp.int32)
    z = r * r
    s = r + r * z * (-1.6666654611e-1 + z * (8.3321608736e-3 + z * -1.9515295891e-4))
    c = 1.0 - 0.5 * z + z * z * (
        4.166664568298827e-2 + z * (-1.388731625493765e-3 + z * 2.443315711809948e-5)
    )
    odd = (quadrant & 1) == 1
    sin = jnp.where(odd, c, s)
    cos = jnp.where(odd, s, c)
    sin = jnp.where((quadrant & 2) == 2, -sin, sin)
    cos = jnp.where(((quadrant + 1) & 2) == 2, -cos, cos)
    return sin, cos


def parts_of(x):
    high = x.astype(jnp.bfloat16)
    low = (x - high.astype(jnp.float32)).astype(jnp.bfloat16)
    return high, low


def window_place(position, patch):
    corner = patch // 4 - ROWS_DEV // 4 - patch // 2 + CSTEP * position
    tile = corner // LANES
    return tile, corner - tile * LANES


def term_of(slab, paths, angle, group, row, col):
    part = slab[0, row : row + SUBS, col : col + LANES] * paths[angle, group, 0]
    for layer in range(1, slab.shape[0]):
        part = part + slab[layer, row : row + SUBS, col : col + LANES] * paths[angle, group, layer]
    return part


def blocks_of(rows, cols):
    wide = cols // LANES
    return [(r // SUBS * wide + c // LANES, r, c) for r in range(0, rows, SUBS) for c in range(0, cols, LANES)]


def terms_kernel(groups, slab_hbm, paths_hbm, jitter_hbm, steps_hbm, *refs):
    terms, factors, scalars = refs[: groups - 1], refs[groups - 1], refs[groups]
    slab, paths, jitter, steps, sems = refs[groups + 1 :]
    group = lax.axis_index("blk")
    column = lax.axis_index("wide")
    columns = lax.axis_size("wide")
    sources = (slab_hbm, paths_hbm, jitter_hbm, steps_hbm)
    copies = [
        pltpu.make_async_copy(source, target, sems.at[i])
        for i, (source, target) in enumerate(zip(sources, (slab, paths, jitter, steps)))
    ]
    for copy in copies:
        copy.start()
    for copy in copies[1:]:
        copy.wait()
    for p in range(jitter.shape[1]):
        scalars[0, p] = jitter[0, p]
        scalars[1, p] = jitter[1, p]
        scalars[2, p] = 0
    second = lax.rem(column, 2)
    scalars[2, 0] = second
    scalars[2, 1] = lax.rem(column // 2, 2)
    scalars[2, 2] = (column >= 2).astype(jnp.int32)
    scalars[2, 3] = (column + 2 < columns).astype(jnp.int32)
    scalars[2, 4] = jnp.where(second == 1, column + 1 < columns, column >= 1).astype(jnp.int32)
    layers, rows, cols = slab.shape
    for step in range(groups):
        source = lax.rem(group - step + groups, groups)
        for layer in range(layers):
            factors[step, layer] = jnp.full((SUBS, LANES), steps[source] * paths[source, group, layer], jnp.float32)
    copies[0].wait()
    for step, term in enumerate(terms):
        angle = lax.rem(group + step + 1, groups)
        for i, r, c in blocks_of(rows, cols):
            term[i] = term_of(slab, paths, angle, group, r, c)


def listed(slab, extra=0):
    _, rows, cols = slab.shape
    return jax.ShapeDtypeStruct((rows // SUBS * (cols // LANES) + extra, SUBS, LANES), jnp.float32)


def slab_terms(slab, paths, jitter, steps, groups):
    vmem = pl.BlockSpec(memory_space=pltpu.VMEM)
    out = pl.pallas_call(
        functools.partial(terms_kernel, groups),
        out_shape=[listed(slab)] * (groups - 1)
        + [
            jax.ShapeDtypeStruct((groups, slab.shape[0], SUBS, LANES), jnp.float32),
            jax.ShapeDtypeStruct((3, jitter.shape[1]), jnp.int32),
        ],
        in_specs=[pl.BlockSpec(memory_space=pltpu.HBM)] * 4,
        out_specs=[vmem] * groups + [pl.BlockSpec(memory_space=pltpu.SMEM)],
        scratch_shapes=[
            pltpu.VMEM(slab.shape, jnp.float32),
            pltpu.SMEM(paths.shape, jnp.float32),
            pltpu.SMEM(jitter.shape, jnp.int32),
            pltpu.SMEM(steps.shape, jnp.float32),
            pltpu.SemaphoreType.DMA((4,)),
        ],
        name="terms",
    )(slab, paths, jitter, steps)
    return out[: groups - 1], out[groups - 1], out[groups]


def own_kernel(slab, paths, tables, term, kept):
    group = lax.axis_index("blk")
    for i, r, c in blocks_of(*slab.shape[1:]):
        term[i] = term_of(slab, paths, group, group, r, c)
    for i in range(tables.shape[0]):
        kept[i] = tables[i]


def own_term(slab, paths, patch):
    vmem = pl.BlockSpec(memory_space=pltpu.VMEM)
    tables = dft_tables(patch)
    return pl.pallas_call(
        own_kernel,
        out_shape=(listed(slab), jax.ShapeDtypeStruct(tables.shape, tables.dtype)),
        in_specs=[vmem, pl.BlockSpec(memory_space=pltpu.SMEM), vmem],
        out_specs=(vmem, vmem),
        compiler_params=pltpu.CompilerParams(vmem_limit_bytes=8 * 1024 * 1024),
        cost_estimate=pl.CostEstimate(flops=2**24, bytes_accessed=2**20, transcendentals=0),
        name="own",
    )(slab, paths, tables)


def update_kernel(count, slab, factors, *refs):
    grads, sums, out, total = refs[:count], refs[count:-2], refs[-2], refs[-1]
    layers, rows, cols = slab.shape
    blocks = grads[0].shape[0]
    value = sums[0][0]
    if len(sums) == 3:
        value = (value + sums[1][0]) + (grads[1][blocks] + sums[2][0])
    total[0, 0] = jnp.sum(value)
    for layer in range(layers):
        for i, r, c in blocks_of(rows, cols):
            value = slab[layer, r : r + SUBS, c : c + LANES]
            for step in range(count):
                value = value - factors[step, layer] * grads[step][i]
            out[layer, r : r + SUBS, c : c + LANES] = value


def updated(slab, factors, grads, sums):
    vmem = pl.BlockSpec(memory_space=pltpu.VMEM)
    return pl.pallas_call(
        functools.partial(update_kernel, len(grads)),
        out_shape=(jax.ShapeDtypeStruct(slab.shape, slab.dtype), jax.ShapeDtypeStruct((1, 1), jnp.float32)),
        in_specs=[vmem] * (2 + len(grads) + len(sums)),
        out_specs=(vmem, pl.BlockSpec(memory_space=pltpu.SMEM)),
        compiler_params=pltpu.CompilerParams(vmem_limit_bytes=8 * 1024 * 1024),
        name="update",
    )(slab, factors, *grads, *sums)


FLAGS = ("second", "lower", "up2", "dn2", "relay")


def prepare_kernel(number, scalars, probe, rolled, frames, twice):
    patch = probe.shape[1]
    for half in range(2):
        for part in range(2):
            twice[part, half * patch : (half + 1) * patch, :] = probe[part]
    for p in range(number):
        _, corner = window_place(p, patch)
        shift = corner + scalars[1, p]
        top = ROWS_DEV // 4 + scalars[0, p]
        start = patch - top
        for part in range(2):
            value = pltpu.roll(twice[part, pl.ds(start, patch), :], shift, 1)
            rolled[p * patch : (p + 1) * patch, part * LANES : (part + 1) * LANES] = value
        frames[p] = jnp.full((SUBS, LANES), shift, jnp.int32)
        frames[number + p] = jnp.full((SUBS, LANES), top, jnp.int32)
    for i in range(len(FLAGS)):
        frames[2 * number + i] = jnp.full((SUBS, LANES), scalars[2, i], jnp.int32)


def prepared(scalars, probe):
    number, patch = scalars.shape[1], probe.shape[1]
    vmem = pl.BlockSpec(memory_space=pltpu.VMEM)
    return pl.pallas_call(
        functools.partial(prepare_kernel, number),
        out_shape=(
            jax.ShapeDtypeStruct((number * patch, 2 * LANES), jnp.float32),
            jax.ShapeDtypeStruct((2 * number + len(FLAGS), SUBS, LANES), jnp.int32),
        ),
        in_specs=[pl.BlockSpec(memory_space=pltpu.SMEM), vmem],
        out_specs=(vmem, vmem),
        scratch_shapes=[pltpu.VMEM((2, 2 * patch, patch), jnp.float32)],
        compiler_params=pltpu.CompilerParams(vmem_limit_bytes=16 * 1024 * 1024),
        cost_estimate=pl.CostEstimate(flops=2**27, bytes_accessed=2**22, transcendentals=0),
        name="prepare",
    )(scalars, probe)


def flag_of(frames, name):
    return frames[frames.shape[0] - len(FLAGS) + FLAGS.index(name)] == 1


def phases_kernel(frames, own, mate, pair, next_pair, real, imag):
    blocks = own.shape[0]
    lower = flag_of(frames, "lower")
    up2_ok = jnp.where(flag_of(frames, "up2"), 1.0, 0.0)
    dn2_ok = jnp.where(flag_of(frames, "dn2"), 1.0, 0.0)
    unused = ROWS_DEV // 4 // SUBS * (blocks * SUBS // ROWS_DEV)
    for i in range(blocks):
        s, c = sin_cos(own[i])
        real[2 * blocks + i], imag[2 * blocks + i] = c, s
        s, c = sin_cos(mate[i])
        real[blocks + i], imag[blocks + i] = c, s
        if i >= unused:
            s, c = sin_cos(jnp.where(lower, pair[i], next_pair[i]))
            real[i], imag[i] = c * up2_ok, s * up2_ok
        if i < blocks - unused:
            s, c = sin_cos(jnp.where(lower, next_pair[i], pair[i]))
            real[4 * blocks + i], imag[4 * blocks + i] = c * dn2_ok, s * dn2_ok


def phases(frames, own, mate, pair, next_pair):
    vmem = pl.BlockSpec(memory_space=pltpu.VMEM)
    out = jax.ShapeDtypeStruct((5 * own.shape[0], SUBS, LANES), jnp.float32)
    return pl.pallas_call(
        phases_kernel,
        out_shape=(out, out),
        in_specs=[vmem] * 5,
        out_specs=(vmem, vmem),
        compiler_params=pltpu.CompilerParams(vmem_limit_bytes=8 * 1024 * 1024),
        cost_estimate=pl.CostEstimate(flops=2**27, bytes_accessed=2**22, transcendentals=0),
        name="phases",
    )(frames, own, mate, pair, next_pair)


def strip_kernel(
    frames,
    here_real,
    here_imag,
    relay,
    rolled,
    measured,
    tables,
    mine,
    to_mate,
    by_pair,
    by_next,
    misfit,
    side_real,
    side_imag,
    wave,
    mid,
    back,
):
    number, patch, _ = measured.shape
    rows = ROWS_DEV
    blocks = relay.shape[0]
    tiles = blocks * SUBS // rows
    near = ROWS_DEV // 4 + JIT
    dot = functools.partial(lax.dot, preferred_element_type=jnp.float32)
    is_second = flag_of(frames, "second")
    is_lower = flag_of(frames, "lower")
    fwd_high, fwd_low, inv_high, inv_low = (tables[i] for i in range(4))

    relay_ok = jnp.where(flag_of(frames, "relay"), 1.0, 0.0)
    for i in range(blocks):
        s, c = sin_cos(relay[i])
        c, s = c * relay_ok, s * relay_ok
        mate_c, mate_s = here_real[blocks + i], here_imag[blocks + i]
        side_real[i] = jnp.where(is_second, mate_c, c)
        side_imag[i] = jnp.where(is_second, mate_s, s)
        side_real[blocks + i] = jnp.where(is_second, c, mate_c)
        side_imag[blocks + i] = jnp.where(is_second, s, mate_s)
    obj_real = (here_real, side_real)
    obj_imag = (here_imag, side_imag)

    lane = lax.broadcasted_iota(jnp.int32, (SUBS, LANES), 1)
    sub = lax.broadcasted_iota(jnp.int32, (SUBS, LANES), 0)

    def masks(p):
        after = lane >= frames[p]
        below = [sub + k * SUBS >= frames[number + p] for k in range(near // SUBS)]
        return after, below

    def pick(refs, p, k, after, below):
        tile, _ = window_place(p, patch)

        def at(row):
            slot, ref = row // rows, refs[0]
            first = row // SUBS * tiles + tile
            if slot in (1, 3):
                ref, first = refs[1], first - (slot + 1) // 2 * blocks
            left = ref[first] if tile >= 0 else 0.0
            right = ref[first + 1] if tile + 1 < tiles else 0.0
            return jnp.where(after, left, right)

        row = k * SUBS
        if row + SUBS <= ROWS_DEV // 4:
            return at(row + patch)
        if row < near:
            return jnp.where(below[k], at(row), at(row + patch))
        return at(row)

    def against(high, low, t_high, t_low):
        return dot(jnp.concatenate([high, low, high], 1), jnp.concatenate([t_high, t_high, t_low], 0))

    def onto(t_high, t_low, high, low):
        return dot(jnp.concatenate([t_high, t_high, t_low], 1), jnp.concatenate([high, low, high], 0))

    steps = patch // SUBS
    for p in range(number):
        after, below = masks(p)
        for k in range(steps):
            o_real = pick(obj_real, p, k, after, below)
            o_imag = pick(obj_imag, p, k, after, below)
            row = p * patch + k * SUBS
            a = rolled[row : row + SUBS, :LANES]
            b = rolled[row : row + SUBS, LANES:]
            wave[row : row + SUBS, :LANES] = a * o_real - b * o_imag
            wave[row : row + SUBS, LANES:] = a * o_imag + b * o_real

    for p in range(0, number, TALL):
        span = slice(p * patch, min(p + TALL, number) * patch)
        high, low = parts_of(wave[span, :])
        mid[span, :] = against(high, low, fwd_high, fwd_low)

    def upright(value):
        count = value.shape[0] // patch
        parts = [
            jnp.concatenate([value[i * patch : (i + 1) * patch, lanes] for i in range(count)], 1)
            for lanes in (slice(0, LANES), slice(LANES, 2 * LANES))
        ]
        return jnp.concatenate(parts, 0)

    total = jnp.zeros((SUBS, LANES), jnp.float32)
    for p in range(0, number, BROAD):
        count = min(BROAD, number - p)
        high, low = parts_of(upright(mid[p * patch : (p + count) * patch, :]))
        spectrum = onto(inv_high, inv_low, high, low)
        real, imag = spectrum[:patch], spectrum[patch:]
        target = jnp.concatenate([measured[p + i] for i in range(count)], 1).astype(jnp.float32)
        power = real * real + imag * imag
        inverse = lax.rsqrt(jnp.maximum(power, 1e-30))
        error = power * inverse - target
        square = error * error
        for k in range(steps):
            for half in range(count):
                total += square[k * SUBS : (k + 1) * SUBS, half * LANES : (half + 1) * LANES]
        ratio = target * jnp.minimum(inverse, FLOOR_RATIO)
        high, low = parts_of(jnp.concatenate([ratio * real, ratio * imag], 0))
        undone = onto(fwd_high, fwd_low, high, low)
        for half in range(count):
            row = (p + half) * patch
            lanes = slice(half * LANES, (half + 1) * LANES)
            back[row : row + patch, :LANES] = undone[:patch, lanes]
            back[row : row + patch, LANES:] = undone[patch:, lanes]
    misfit[0] = total

    for p in range(0, number, TALL):
        span = slice(p * patch, min(p + TALL, number) * patch)
        high, low = parts_of(back[span, :])
        out = against(high, low, inv_high, inv_low)
        w = wave[span, :]
        mid[span, :LANES] = w[:, :LANES] * out[:, LANES:] - w[:, LANES:] * out[:, :LANES]

    grads = {}
    for t in range(tiles):
        meets = []
        for p in range(number):
            tile, _ = window_place(p, patch)
            if t in (tile, tile + 1):
                after, below = masks(p)
                meets.append((p, after if t == tile else jnp.logical_not(after), below))
        for k in range(steps):
            row = k * SUBS
            here = there = None
            for p, mask, below in meets:
                term = jnp.where(mask, mid[p * patch + row : p * patch + row + SUBS, :LANES], 0.0)
                if row + SUBS <= ROWS_DEV // 4:
                    there = term if there is None else there + term
                elif row < near:
                    kept = jnp.where(below[k], term, 0.0)
                    here = kept if here is None else here + kept
                    there = (term - kept) if there is None else there + (term - kept)
                else:
                    here = term if here is None else here + term
            grads[k, t] = here
            grads[k + steps, t] = there

    def add_to(slot, r, t):
        value = grads.get((slot * (rows // SUBS) + r // SUBS, t))
        return jnp.zeros((SUBS, LANES), jnp.float32) if value is None else value

    for i, r, c in blocks_of(rows, tiles * LANES):
        up2, up1, here, dn1, dn2 = (add_to(slot, r, c // LANES) for slot in range(5))
        mine[i] = here
        to_mate[i] = jnp.where(is_second, up1, dn1)
        to_mate[blocks + i] = jnp.where(is_second, dn1, up1)
        by_pair[i] = jnp.where(is_lower, up2, dn2)
        by_next[i] = jnp.where(is_lower, dn2, up2)


def strip_gradient(frames, here, relay, rolled, measured, tables):
    number, patch, _ = measured.shape
    blocks = relay.shape[0]
    vmem = pl.BlockSpec(memory_space=pltpu.VMEM)

    def block_list(count):
        return jax.ShapeDtypeStruct((count, SUBS, LANES), jnp.float32)

    return pl.pallas_call(
        strip_kernel,
        out_shape=tuple(block_list(n) for n in (blocks, 2 * blocks, blocks, blocks, 1)),
        in_specs=[vmem] * 7,
        out_specs=(vmem,) * 5,
        scratch_shapes=[
            pltpu.VMEM((2 * blocks, SUBS, LANES), jnp.float32),
            pltpu.VMEM((2 * blocks, SUBS, LANES), jnp.float32),
            pltpu.VMEM((number * patch, 2 * LANES), jnp.float32),
            pltpu.VMEM((number * patch, 2 * LANES), jnp.float32),
            pltpu.VMEM((number * patch, 2 * LANES), jnp.float32),
        ],
        compiler_params=pltpu.CompilerParams(vmem_limit_bytes=40 * 1024 * 1024),
        cost_estimate=pl.CostEstimate(
            flops=24 * number * patch**3 * 4, bytes_accessed=4 * number * patch * patch, transcendentals=0
        ),
        name="strip",
    )(frames, *here, relay, rolled, measured, tables)


def permuted(value, axis, target):
    count = lax.axis_size(axis)
    pairs = [(i, target(i)) for i in range(count) if 0 <= target(i) < count]
    return lax.ppermute(value, axis, pairs)


def with_mate(value):
    return permuted(value, "wide", lambda i: i ^ 1)


def with_pair(value):
    return permuted(value, "wide", lambda i: i ^ 2)


def across(value):
    count = lax.axis_size("wide")

    def target(i):
        j = i + 2 if i // 2 % 2 else i - 2
        return j if 0 <= j < count else i ^ 1

    return permuted(value, "wide", target)


def joined(value, axis, steps):
    for step in steps:
        value = value + permuted(value, axis, lambda i: i ^ step)
    return value


def program(volume, path_lengths, probe, measured, jitter, step_sizes):
    groups = lax.axis_size("blk")
    column = lax.axis_index("wide")
    columns = lax.axis_size("wide")
    slab = volume[0]

    def to_group(value, step):
        return lax.ppermute(value, "blk", [(i, (i + step) % groups) for i in range(groups)])

    terms, factors, scalars = slab_terms(slab, path_lengths, jitter[:, 0, 0], step_sizes, groups)
    own, tables = own_term(slab, path_lengths, probe.shape[-1])
    for step in range(1, groups):
        own = own + to_group(terms[step - 1], step)

    even = column % 2 == column // 2 % 2
    next_pair = across(own)
    pair = with_pair(own)
    mate = with_mate(own)
    rolled, frames = prepared(scalars, probe)
    relay = with_mate(jnp.where(even, pair, next_pair))
    here = phases(frames, own, mate, pair, next_pair)
    blocks = own.shape[0]
    mine, to_mate, by_pair, by_next, local = strip_gradient(frames, here, relay, rolled, measured[0, 0], tables)
    got = with_mate(to_mate)
    if groups != 2:
        local = joined(local, "blk", [2**k for k in range(groups.bit_length() - 1)])
    local = joined(local, "wide", [4])
    mine = mine + got[:blocks]
    passed = got[blocks:]
    zero = jnp.zeros_like(passed)
    from_pair = with_pair(by_pair + jnp.where(even, passed, zero))
    from_next = across(by_next + jnp.where(even, zero, passed))
    local = joined(local, "wide", [1])
    local = joined(local, "wide", [2**k for k in range(3, columns.bit_length() - 1)])
    gradient = mine + (from_next + from_pair)
    grads = [gradient]
    if groups == 2:
        grads.append(to_group(jnp.concatenate([gradient, local], 0), 1))
        sums = [local, with_pair(local)]
        pairs = [(i, (i + columns) % (2 * columns) ^ 2) for i in range(2 * columns)]
        sums.append(lax.ppermute(local, ("blk", "wide"), pairs))
    else:
        for step in range(1, groups):
            grads.append(to_group(gradient, step))
        sums = [joined(local, "wide", [2])]
    new, total = updated(slab, factors, grads, sums)
    return (new[None], total[0, 0])


def solution(mesh):
    in_specs = (
        P("blk", None, "wide", None),
        P(),
        P(),
        P("blk", "wide", None, None, None),
        P(None, "blk", "wide", None),
        P(),
    )
    out_specs = (P("blk", None, "wide", None), P())
    return jax.shard_map(program, mesh=mesh, in_specs=in_specs, out_specs=out_specs, check_vma=False)
```

```python
import functools
import math

import jax
import jax.numpy as jnp
import numpy as np
from jax import lax
from jax.experimental import pallas as pl
from jax.experimental.pallas import tpu as pltpu
from jax.sharding import PartitionSpec as P

ROWS_DEV = 32
CSTEP = 64
JIT = 16
FLOOR_RATIO = 4.0
LANES = 128
TALL = 4
SIDE = 14
BROAD = 2
SUBS = 8
HALF_PI = (1.5703125, 4.837512969970703125e-4, 7.54978995489188216e-8)


def dft_tables(length):
    grid = np.arange(length)
    angles = (grid[:, None] * grid[None, :] % length) * (2.0 * math.pi / length)
    cos = np.cos(angles) / math.sqrt(length)
    sin = -np.sin(angles) / math.sqrt(length)
    table = np.block([[cos, sin], [-sin, cos]])
    high = table.astype(jnp.bfloat16)
    low = (table - high.astype(np.float64)).astype(jnp.bfloat16)
    return np.stack([high, low, high.T, low.T])


def sin_cos(x):
    turns = jnp.floor(x * (2.0 / math.pi) + 0.5)
    r = x - turns * HALF_PI[0]
    r = r - turns * HALF_PI[1]
    r = r - turns * HALF_PI[2]
    quadrant = turns.astype(jnp.int32)
    z = r * r
    s = r + r * z * (-1.6666654611e-1 + z * (8.3321608736e-3 + z * -1.9515295891e-4))
    c = 1.0 - 0.5 * z + z * z * (
        4.166664568298827e-2 + z * (-1.388731625493765e-3 + z * 2.443315711809948e-5)
    )
    odd = (quadrant & 1) == 1
    sin = jnp.where(odd, c, s)
    cos = jnp.where(odd, s, c)
    sin = jnp.where((quadrant & 2) == 2, -sin, sin)
    cos = jnp.where(((quadrant + 1) & 2) == 2, -cos, cos)
    return sin, cos


def parts_of(x):
    high = x.astype(jnp.bfloat16)
    low = (x - high.astype(jnp.float32)).astype(jnp.bfloat16)
    return high, low


def window_place(position, patch):
    corner = patch // 4 - ROWS_DEV // 4 - patch // 2 + CSTEP * position
    tile = corner // LANES
    return tile, corner - tile * LANES


def term_of(slab, paths, angle, group, row, col):
    part = slab[0, row : row + SUBS, col : col + LANES] * paths[angle, group, 0]
    for layer in range(1, slab.shape[0]):
        part = part + slab[layer, row : row + SUBS, col : col + LANES] * paths[angle, group, layer]
    return part


def blocks_of(rows, cols):
    wide = cols // LANES
    return [(r // SUBS * wide + c // LANES, r, c) for r in range(0, rows, SUBS) for c in range(0, cols, LANES)]


def terms_kernel(groups, slab_hbm, paths_hbm, jitter_hbm, steps_hbm, *refs):
    terms, factors, scalars = refs[: groups - 1], refs[groups - 1], refs[groups]
    slab, paths, jitter, steps, sems = refs[groups + 1 :]
    group = lax.axis_index("blk")
    column = lax.axis_index("wide")
    columns = lax.axis_size("wide")
    sources = (slab_hbm, paths_hbm, jitter_hbm, steps_hbm)
    copies = [
        pltpu.make_async_copy(source, target, sems.at[i])
        for i, (source, target) in enumerate(zip(sources, (slab, paths, jitter, steps)))
    ]
    for copy in copies:
        copy.start()
    for copy in copies[1:]:
        copy.wait()
    for p in range(jitter.shape[1]):
        scalars[0, p] = jitter[0, p]
        scalars[1, p] = jitter[1, p]
        scalars[2, p] = 0
    second = lax.rem(column, 2)
    scalars[2, 0] = second
    scalars[2, 1] = lax.rem(column // 2, 2)
    scalars[2, 2] = (column >= 2).astype(jnp.int32)
    scalars[2, 3] = (column + 2 < columns).astype(jnp.int32)
    scalars[2, 4] = jnp.where(second == 1, column + 1 < columns, column >= 1).astype(jnp.int32)
    layers, rows, cols = slab.shape
    for step in range(groups):
        source = lax.rem(group - step + groups, groups)
        for layer in range(layers):
            factors[step, layer] = jnp.full((SUBS, LANES), steps[source] * paths[source, group, layer], jnp.float32)
    copies[0].wait()
    for step, term in enumerate(terms):
        angle = lax.rem(group + step + 1, groups)
        for i, r, c in blocks_of(rows, cols):
            term[i] = term_of(slab, paths, angle, group, r, c)


def listed(slab, extra=0):
    _, rows, cols = slab.shape
    return jax.ShapeDtypeStruct((rows // SUBS * (cols // LANES) + extra, SUBS, LANES), jnp.float32)


def slab_terms(slab, paths, jitter, steps, groups):
    vmem = pl.BlockSpec(memory_space=pltpu.VMEM)
    out = pl.pallas_call(
        functools.partial(terms_kernel, groups),
        out_shape=[listed(slab)] * (groups - 1)
        + [
            jax.ShapeDtypeStruct((groups, slab.shape[0], SUBS, LANES), jnp.float32),
            jax.ShapeDtypeStruct((3, jitter.shape[1]), jnp.int32),
        ],
        in_specs=[pl.BlockSpec(memory_space=pltpu.HBM)] * 4,
        out_specs=[vmem] * groups + [pl.BlockSpec(memory_space=pltpu.SMEM)],
        scratch_shapes=[
            pltpu.VMEM(slab.shape, jnp.float32),
            pltpu.SMEM(paths.shape, jnp.float32),
            pltpu.SMEM(jitter.shape, jnp.int32),
            pltpu.SMEM(steps.shape, jnp.float32),
            pltpu.SemaphoreType.DMA((4,)),
        ],
        name="terms",
    )(slab, paths, jitter, steps)
    return out[: groups - 1], out[groups - 1], out[groups]


def own_kernel(slab, paths, tables, term, kept):
    group = lax.axis_index("blk")
    for i, r, c in blocks_of(*slab.shape[1:]):
        term[i] = term_of(slab, paths, group, group, r, c)
    for i in range(tables.shape[0]):
        kept[i] = tables[i]


def own_term(slab, paths, patch):
    vmem = pl.BlockSpec(memory_space=pltpu.VMEM)
    tables = dft_tables(patch)
    return pl.pallas_call(
        own_kernel,
        out_shape=(listed(slab), jax.ShapeDtypeStruct(tables.shape, tables.dtype)),
        in_specs=[vmem, pl.BlockSpec(memory_space=pltpu.SMEM), vmem],
        out_specs=(vmem, vmem),
        compiler_params=pltpu.CompilerParams(vmem_limit_bytes=8 * 1024 * 1024),
        cost_estimate=pl.CostEstimate(flops=2**24, bytes_accessed=2**20, transcendentals=0),
        name="own",
    )(slab, paths, tables)


def update_kernel(count, slab, factors, *refs):
    grads, sums, out, total = refs[:count], refs[count:-2], refs[-2], refs[-1]
    layers, rows, cols = slab.shape
    blocks = grads[0].shape[0]
    value = sums[0][0]
    if len(sums) == 3:
        value = (value + sums[1][0]) + (grads[1][blocks] + sums[2][0])
    total[0, 0] = jnp.sum(value)
    for layer in range(layers):
        for i, r, c in blocks_of(rows, cols):
            value = slab[layer, r : r + SUBS, c : c + LANES]
            for step in range(count):
                value = value - factors[step, layer] * grads[step][i]
            out[layer, r : r + SUBS, c : c + LANES] = value


def updated(slab, factors, grads, sums):
    vmem = pl.BlockSpec(memory_space=pltpu.VMEM)
    return pl.pallas_call(
        functools.partial(update_kernel, len(grads)),
        out_shape=(jax.ShapeDtypeStruct(slab.shape, slab.dtype), jax.ShapeDtypeStruct((1, 1), jnp.float32)),
        in_specs=[vmem] * (2 + len(grads) + len(sums)),
        out_specs=(vmem, pl.BlockSpec(memory_space=pltpu.SMEM)),
        compiler_params=pltpu.CompilerParams(vmem_limit_bytes=8 * 1024 * 1024),
        name="update",
    )(slab, factors, *grads, *sums)


FLAGS = ("second", "lower", "up2", "dn2", "relay")


def prepare_kernel(number, scalars, probe, rolled, frames, twice):
    patch = probe.shape[1]
    for half in range(2):
        for part in range(2):
            twice[part, half * patch : (half + 1) * patch, :] = probe[part]
    for p in range(number):
        _, corner = window_place(p, patch)
        shift = corner + scalars[1, p]
        top = ROWS_DEV // 4 + scalars[0, p]
        start = patch - top
        for part in range(2):
            value = pltpu.roll(twice[part, pl.ds(start, patch), :], shift, 1)
            rolled[p * patch : (p + 1) * patch, part * LANES : (part + 1) * LANES] = value
        frames[p] = jnp.full((SUBS, LANES), shift, jnp.int32)
        frames[number + p] = jnp.full((SUBS, LANES), top, jnp.int32)
    for i in range(len(FLAGS)):
        frames[2 * number + i] = jnp.full((SUBS, LANES), scalars[2, i], jnp.int32)


def prepared(scalars, probe):
    number, patch = scalars.shape[1], probe.shape[1]
    vmem = pl.BlockSpec(memory_space=pltpu.VMEM)
    return pl.pallas_call(
        functools.partial(prepare_kernel, number),
        out_shape=(
            jax.ShapeDtypeStruct((number * patch, 2 * LANES), jnp.float32),
            jax.ShapeDtypeStruct((2 * number + len(FLAGS), SUBS, LANES), jnp.int32),
        ),
        in_specs=[pl.BlockSpec(memory_space=pltpu.SMEM), vmem],
        out_specs=(vmem, vmem),
        scratch_shapes=[pltpu.VMEM((2, 2 * patch, patch), jnp.float32)],
        compiler_params=pltpu.CompilerParams(vmem_limit_bytes=16 * 1024 * 1024),
        cost_estimate=pl.CostEstimate(flops=2**27, bytes_accessed=2**22, transcendentals=0),
        name="prepare",
    )(scalars, probe)


def flag_of(frames, name):
    return frames[frames.shape[0] - len(FLAGS) + FLAGS.index(name)] == 1


def frame_masks(frames, number, p):
    lane = lax.broadcasted_iota(jnp.int32, (SUBS, LANES), 1)
    sub = lax.broadcasted_iota(jnp.int32, (SUBS, LANES), 0)
    near = ROWS_DEV // 4 + JIT
    return lane >= frames[p], [sub + k * SUBS >= frames[number + p] for k in range(near // SUBS)]


def object_at(ref, first_block, row_block, p, patch, tiles, after):
    tile, _ = window_place(p, patch)
    first = first_block + row_block * tiles + tile
    left = ref[first] if tile >= 0 else 0.0
    right = ref[first + 1] if tile + 1 < tiles else 0.0
    return jnp.where(after, left, right)


def put_wave(wave, rolled, row, source, real, imag):
    a, b = rolled[pl.ds(source, SUBS), :LANES], rolled[pl.ds(source, SUBS), LANES:]
    wave[row : row + SUBS, :LANES] = a * real - b * imag
    wave[row : row + SUBS, LANES:] = a * imag + b * real


def against(high, low, t_high, t_low):
    left = jnp.concatenate([high, low, high], 1)
    return lax.dot(left, jnp.concatenate([t_high, t_high, t_low], 0), preferred_element_type=jnp.float32)


def onto(t_high, t_low, high, low):
    right = jnp.concatenate([high, low, high], 0)
    return lax.dot(jnp.concatenate([t_high, t_high, t_low], 1), right, preferred_element_type=jnp.float32)


def side_rows():
    second = lax.rem(lax.axis_index("wide"), 2)
    upper, lower = ROWS_DEV, 3 * ROWS_DEV
    return jnp.where(second == 1, upper, lower), jnp.where(second == 1, lower, upper)


def ahead_kernel(frames, own, mate, pair, next_pair, rolled, tables, wave, mid, real, imag):
    blocks = own.shape[0]
    patch = rolled.shape[1] // 2
    number = rolled.shape[0] // patch
    tiles = blocks * SUBS // ROWS_DEV
    steps = ROWS_DEV // SUBS
    lower = flag_of(frames, "lower")
    up2_ok = jnp.where(flag_of(frames, "up2"), 1.0, 0.0)
    dn2_ok = jnp.where(flag_of(frames, "dn2"), 1.0, 0.0)
    unused = ROWS_DEV // 4 // SUBS * tiles
    for i in range(blocks):
        if i >= unused:
            s, c = sin_cos(jnp.where(lower, pair[i], next_pair[i]))
            real[i], imag[i] = c * up2_ok, s * up2_ok
        if i < blocks - unused:
            s, c = sin_cos(jnp.where(lower, next_pair[i], pair[i]))
            real[blocks + i], imag[blocks + i] = c * dn2_ok, s * dn2_ok
        s, c = sin_cos(own[i])
        real[2 * blocks + i], imag[2 * blocks + i] = c, s
        s, c = sin_cos(mate[i])
        real[3 * blocks + i], imag[3 * blocks + i] = c, s

    mate_row, _ = side_rows()
    near = ROWS_DEV // 4 + JIT
    t_high, t_low = tables[0], tables[1]
    for p in range(number):
        after, below = frame_masks(frames, number, p)
        place = (p, patch, tiles, after)
        for k in range(steps):
            row = k * SUBS
            parts = []
            for ref in (real, imag):
                if row + SUBS <= ROWS_DEV // 4:
                    parts.append(object_at(ref, blocks, k, *place))
                elif row < near:
                    up = object_at(ref, 0, k, *place)
                    parts.append(jnp.where(below[k], up, object_at(ref, blocks, k, *place)))
                else:
                    parts.append(object_at(ref, 0, k, *place))
            put_wave(wave, rolled, p * patch + row, p * patch + row, *parts)
            parts = [object_at(ref, 2 * blocks, k, *place) for ref in (real, imag)]
            row += p * patch + 2 * ROWS_DEV
            put_wave(wave, rolled, row, row, *parts)
            row = k * SUBS
            parts = [object_at(ref, 3 * blocks, k, *place) for ref in (real, imag)]
            source = pl.multiple_of(p * patch + mate_row + row, SUBS)
            put_wave(wave, rolled, p * patch + ROWS_DEV + row, source, *parts)

    here = 3 * ROWS_DEV
    for p in range(0, number, TALL):
        windows = range(p, min(p + TALL, number))
        value = jnp.concatenate([wave[q * patch : q * patch + here, :] for q in windows], 0)
        out = against(*parts_of(value), t_high, t_low)
        for i, q in enumerate(windows):
            mid[q * patch : q * patch + here, :] = out[i * here : (i + 1) * here]


def ahead(frames, own, mate, pair, next_pair, rolled, tables):
    vmem = pl.BlockSpec(memory_space=pltpu.VMEM)
    out = jax.ShapeDtypeStruct(rolled.shape, jnp.float32)
    scratch = pltpu.VMEM((4 * own.shape[0], SUBS, LANES), jnp.float32)
    return pl.pallas_call(
        ahead_kernel,
        out_shape=(out, out),
        in_specs=[vmem] * 7,
        out_specs=(vmem, vmem),
        scratch_shapes=[scratch, scratch],
        compiler_params=pltpu.CompilerParams(vmem_limit_bytes=24 * 1024 * 1024),
        cost_estimate=pl.CostEstimate(flops=2**27, bytes_accessed=2**22, transcendentals=0),
        name="ahead",
    )(frames, own, mate, pair, next_pair, rolled, tables)


def strip_kernel(
    frames,
    wave,
    mid,
    relay,
    rolled,
    measured,
    tables,
    mine,
    to_mate,
    by_pair,
    by_next,
    misfit,
    real,
    imag,
    side_wave,
    side_mid,
    back,
    terms,
):
    number, patch, _ = measured.shape
    rows = ROWS_DEV
    blocks = relay.shape[0]
    tiles = blocks * SUBS // rows
    steps = patch // SUBS
    near = ROWS_DEV // 4 + JIT
    is_second = flag_of(frames, "second")
    is_lower = flag_of(frames, "lower")
    fwd_high, fwd_low, inv_high, inv_low = (tables[i] for i in range(4))

    relay_ok = jnp.where(flag_of(frames, "relay"), 1.0, 0.0)
    for i in range(blocks):
        s, c = sin_cos(relay[i])
        real[i], imag[i] = c * relay_ok, s * relay_ok
    _, relay_row = side_rows()
    for p in range(number):
        after, _ = frame_masks(frames, number, p)
        for k in range(rows // SUBS):
            parts = [object_at(ref, 0, k, p, patch, tiles, after) for ref in (real, imag)]
            source = pl.multiple_of(p * patch + relay_row + k * SUBS, SUBS)
            put_wave(side_wave, rolled, p * rows + k * SUBS, source, *parts)
    for p in range(0, number, SIDE):
        span = slice(p * rows, min(p + SIDE, number) * rows)
        side_mid[span, :] = against(*parts_of(side_wave[span, :]), fwd_high, fwd_low)
    second = relay_row > 2 * rows

    def window_rows(whole, side, p):
        at = p * patch
        mates, others = whole[at + rows : at + 2 * rows, :], side[p * rows : (p + 1) * rows, :]
        upper, lower = jnp.where(second, mates, others), jnp.where(second, others, mates)
        return jnp.concatenate([whole[at : at + rows, :], upper, whole[at + 2 * rows : at + 3 * rows, :], lower], 0)

    def upright(value):
        count = value.shape[0] // patch
        parts = [
            jnp.concatenate([value[i * patch : (i + 1) * patch, lanes] for i in range(count)], 1)
            for lanes in (slice(0, LANES), slice(LANES, 2 * LANES))
        ]
        return jnp.concatenate(parts, 0)

    total = jnp.zeros((SUBS, LANES), jnp.float32)
    for p in range(0, number, BROAD):
        count = min(BROAD, number - p)
        high, low = parts_of(upright(jnp.concatenate([window_rows(mid, side_mid, p + i) for i in range(count)], 0)))
        spectrum = onto(inv_high, inv_low, high, low)
        real, imag = spectrum[:patch], spectrum[patch:]
        target = jnp.concatenate([measured[p + i] for i in range(count)], 1).astype(jnp.float32)
        power = real * real + imag * imag
        inverse = lax.rsqrt(jnp.maximum(power, 1e-30))
        error = power * inverse - target
        square = error * error
        for k in range(steps):
            for half in range(count):
                total += square[k * SUBS : (k + 1) * SUBS, half * LANES : (half + 1) * LANES]
        ratio = target * jnp.minimum(inverse, FLOOR_RATIO)
        high, low = parts_of(jnp.concatenate([ratio * real, ratio * imag], 0))
        undone = onto(fwd_high, fwd_low, high, low)
        for half in range(count):
            row = (p + half) * patch
            lanes = slice(half * LANES, (half + 1) * LANES)
            back[row : row + patch, :LANES] = undone[:patch, lanes]
            back[row : row + patch, LANES:] = undone[patch:, lanes]
    misfit[0] = total

    for p in range(0, number, TALL):
        span = slice(p * patch, min(p + TALL, number) * patch)
        high, low = parts_of(back[span, :])
        out = against(high, low, inv_high, inv_low)
        windows = range(p, min(p + TALL, number))
        w = jnp.concatenate([window_rows(wave, side_wave, q) for q in windows], 0)
        terms[span, :] = w[:, :LANES] * out[:, LANES:] - w[:, LANES:] * out[:, :LANES]

    grads = {}
    for t in range(tiles):
        meets = []
        for p in range(number):
            tile, _ = window_place(p, patch)
            if t in (tile, tile + 1):
                after, below = frame_masks(frames, number, p)
                meets.append((p, after if t == tile else jnp.logical_not(after), below))
        for k in range(steps):
            row = k * SUBS
            here = there = None
            for p, mask, below in meets:
                term = jnp.where(mask, terms[p * patch + row : p * patch + row + SUBS, :], 0.0)
                if row + SUBS <= ROWS_DEV // 4:
                    there = term if there is None else there + term
                elif row < near:
                    kept = jnp.where(below[k], term, 0.0)
                    here = kept if here is None else here + kept
                    there = (term - kept) if there is None else there + (term - kept)
                else:
                    here = term if here is None else here + term
            grads[k, t] = here
            grads[k + steps, t] = there

    def add_to(slot, r, t):
        value = grads.get((slot * (rows // SUBS) + r // SUBS, t))
        return jnp.zeros((SUBS, LANES), jnp.float32) if value is None else value

    for i, r, c in blocks_of(rows, tiles * LANES):
        up2, up1, here, dn1, dn2 = (add_to(slot, r, c // LANES) for slot in range(5))
        mine[i] = here
        to_mate[i] = jnp.where(is_second, up1, dn1)
        to_mate[blocks + i] = jnp.where(is_second, dn1, up1)
        by_pair[i] = jnp.where(is_lower, up2, dn2)
        by_next[i] = jnp.where(is_lower, dn2, up2)


def strip_gradient(frames, wave, mid, relay, rolled, measured, tables):
    number, patch, _ = measured.shape
    blocks = relay.shape[0]
    vmem = pl.BlockSpec(memory_space=pltpu.VMEM)

    def block_list(count):
        return jax.ShapeDtypeStruct((count, SUBS, LANES), jnp.float32)

    side = pltpu.VMEM((number * ROWS_DEV, 2 * LANES), jnp.float32)
    return pl.pallas_call(
        strip_kernel,
        out_shape=tuple(block_list(n) for n in (blocks, 2 * blocks, blocks, blocks, 1)),
        in_specs=[vmem] * 7,
        out_specs=(vmem,) * 5,
        scratch_shapes=[
            pltpu.VMEM((blocks, SUBS, LANES), jnp.float32),
            pltpu.VMEM((blocks, SUBS, LANES), jnp.float32),
            side,
            side,
            pltpu.VMEM((number * patch, 2 * LANES), jnp.float32),
            pltpu.VMEM((number * patch, LANES), jnp.float32),
        ],
        compiler_params=pltpu.CompilerParams(vmem_limit_bytes=40 * 1024 * 1024),
        cost_estimate=pl.CostEstimate(
            flops=24 * number * patch**3 * 4, bytes_accessed=4 * number * patch * patch, transcendentals=0
        ),
        name="strip",
    )(frames, wave, mid, relay, rolled, measured, tables)


def permuted(value, axis, target):
    count = lax.axis_size(axis)
    pairs = [(i, target(i)) for i in range(count) if 0 <= target(i) < count]
    return lax.ppermute(value, axis, pairs)


def with_mate(value):
    return permuted(value, "wide", lambda i: i ^ 1)


def with_pair(value):
    return permuted(value, "wide", lambda i: i ^ 2)


def across(value):
    count = lax.axis_size("wide")

    def target(i):
        j = i + 2 if i // 2 % 2 else i - 2
        return j if 0 <= j < count else i ^ 1

    return permuted(value, "wide", target)


def joined(value, axis, steps):
    for step in steps:
        value = value + permuted(value, axis, lambda i: i ^ step)
    return value


def program(volume, path_lengths, probe, measured, jitter, step_sizes):
    groups = lax.axis_size("blk")
    column = lax.axis_index("wide")
    columns = lax.axis_size("wide")
    slab = volume[0]

    def to_group(value, step):
        return lax.ppermute(value, "blk", [(i, (i + step) % groups) for i in range(groups)])

    terms, factors, scalars = slab_terms(slab, path_lengths, jitter[:, 0, 0], step_sizes, groups)
    own, tables = own_term(slab, path_lengths, probe.shape[-1])
    for step in range(1, groups):
        own = own + to_group(terms[step - 1], step)

    even = column % 2 == column // 2 % 2
    next_pair = across(own)
    pair = with_pair(own)
    mate = with_mate(own)
    rolled, frames = prepared(scalars, probe)
    relay = with_mate(jnp.where(even, pair, next_pair))
    wave, mid = ahead(frames, own, mate, pair, next_pair, rolled, tables)
    blocks = own.shape[0]
    mine, to_mate, by_pair, by_next, local = strip_gradient(frames, wave, mid, relay, rolled, measured[0, 0], tables)
    got = with_mate(to_mate)
    if groups != 2:
        local = joined(local, "blk", [2**k for k in range(groups.bit_length() - 1)])
    local = joined(local, "wide", [4])
    mine = mine + got[:blocks]
    passed = got[blocks:]
    zero = jnp.zeros_like(passed)
    from_pair = with_pair(by_pair + jnp.where(even, passed, zero))
    from_next = across(by_next + jnp.where(even, zero, passed))
    local = joined(local, "wide", [1])
    local = joined(local, "wide", [2**k for k in range(3, columns.bit_length() - 1)])
    gradient = mine + (from_next + from_pair)
    grads = [gradient]
    if groups == 2:
        grads.append(to_group(jnp.concatenate([gradient, local], 0), 1))
        sums = [local, with_pair(local)]
        pairs = [(i, (i + columns) % (2 * columns) ^ 2) for i in range(2 * columns)]
        sums.append(lax.ppermute(local, ("blk", "wide"), pairs))
    else:
        for step in range(1, groups):
            grads.append(to_group(gradient, step))
        sums = [joined(local, "wide", [2])]
    new, total = updated(slab, factors, grads, sums)
    return (new[None], total[0, 0])


def solution(mesh):
    in_specs = (
        P("blk", None, "wide", None),
        P(),
        P(),
        P("blk", "wide", None, None, None),
        P(None, "blk", "wide", None),
        P(),
    )
    out_specs = (P("blk", None, "wide", None), P())
    return jax.shard_map(program, mesh=mesh, in_specs=in_specs, out_specs=out_specs, check_vma=False)
```

```python
import functools
import math

import jax
import jax.numpy as jnp
import numpy as np
from jax import lax
from jax.experimental import pallas as pl
from jax.experimental.pallas import tpu as pltpu
from jax.sharding import PartitionSpec as P

ROWS_DEV = 32
CSTEP = 64
JIT = 16
FLOOR_RATIO = 4.0
LANES = 128
TALL = 2
SIDE = 7
BROAD = 2
SUBS = 8
HALF_PI = (1.5703125, 4.837512969970703125e-4, 7.54978995489188216e-8)


def dft_tables(length):
    grid = np.arange(length)
    angles = (grid[:, None] * grid[None, :] % length) * (2.0 * math.pi / length)
    cos = np.cos(angles) / math.sqrt(length)
    sin = -np.sin(angles) / math.sqrt(length)
    table = np.block([[cos, sin], [-sin, cos]])
    high = table.astype(jnp.bfloat16)
    low = (table - high.astype(np.float64)).astype(jnp.bfloat16)
    return np.stack([high, low, high.T, low.T])


def sin_cos(x):
    turns = jnp.floor(x * (2.0 / math.pi) + 0.5)
    r = x - turns * HALF_PI[0]
    r = r - turns * HALF_PI[1]
    r = r - turns * HALF_PI[2]
    quadrant = turns.astype(jnp.int32)
    z = r * r
    s = r + r * z * (-1.6666654611e-1 + z * (8.3321608736e-3 + z * -1.9515295891e-4))
    c = 1.0 - 0.5 * z + z * z * (
        4.166664568298827e-2 + z * (-1.388731625493765e-3 + z * 2.443315711809948e-5)
    )
    odd = (quadrant & 1) == 1
    sin = jnp.where(odd, c, s)
    cos = jnp.where(odd, s, c)
    sin = jnp.where((quadrant & 2) == 2, -sin, sin)
    cos = jnp.where(((quadrant + 1) & 2) == 2, -cos, cos)
    return sin, cos


def parts_of(x):
    high = x.astype(jnp.bfloat16)
    low = (x - high.astype(jnp.float32)).astype(jnp.bfloat16)
    return high, low


def window_place(position, patch):
    corner = patch // 4 - ROWS_DEV // 4 - patch // 2 + CSTEP * position
    tile = corner // LANES
    return tile, corner - tile * LANES


def term_of(slab, paths, angle, group, row, col):
    part = slab[0, row : row + SUBS, col : col + LANES] * paths[angle, group, 0]
    for layer in range(1, slab.shape[0]):
        part = part + slab[layer, row : row + SUBS, col : col + LANES] * paths[angle, group, layer]
    return part


def blocks_of(rows, cols):
    wide = cols // LANES
    return [(r // SUBS * wide + c // LANES, r, c) for r in range(0, rows, SUBS) for c in range(0, cols, LANES)]


def terms_kernel(groups, slab_hbm, paths_hbm, jitter_hbm, steps_hbm, *refs):
    terms, factors, scalars = refs[: groups - 1], refs[groups - 1], refs[groups]
    slab, paths, jitter, steps, sems = refs[groups + 1 :]
    group = lax.axis_index("blk")
    column = lax.axis_index("wide")
    columns = lax.axis_size("wide")
    sources = (slab_hbm, paths_hbm, jitter_hbm, steps_hbm)
    copies = [
        pltpu.make_async_copy(source, target, sems.at[i])
        for i, (source, target) in enumerate(zip(sources, (slab, paths, jitter, steps)))
    ]
    for copy in copies:
        copy.start()
    for copy in copies[1:]:
        copy.wait()
    for p in range(jitter.shape[1]):
        scalars[0, p] = jitter[0, p]
        scalars[1, p] = jitter[1, p]
        scalars[2, p] = 0
    second = lax.rem(column, 2)
    scalars[2, 0] = second
    scalars[2, 1] = lax.rem(column // 2, 2)
    scalars[2, 2] = (column >= 2).astype(jnp.int32)
    scalars[2, 3] = (column + 2 < columns).astype(jnp.int32)
    scalars[2, 4] = jnp.where(second == 1, column + 1 < columns, column >= 1).astype(jnp.int32)
    layers, rows, cols = slab.shape
    for step in range(groups):
        source = lax.rem(group - step + groups, groups)
        for layer in range(layers):
            factors[step, layer] = jnp.full((SUBS, LANES), steps[source] * paths[source, group, layer], jnp.float32)
    copies[0].wait()
    for step, term in enumerate(terms):
        angle = lax.rem(group + step + 1, groups)
        for i, r, c in blocks_of(rows, cols):
            term[i] = term_of(slab, paths, angle, group, r, c)


def listed(slab, extra=0):
    _, rows, cols = slab.shape
    return jax.ShapeDtypeStruct((rows // SUBS * (cols // LANES) + extra, SUBS, LANES), jnp.float32)


def slab_terms(slab, paths, jitter, steps, groups):
    vmem = pl.BlockSpec(memory_space=pltpu.VMEM)
    out = pl.pallas_call(
        functools.partial(terms_kernel, groups),
        out_shape=[listed(slab)] * (groups - 1)
        + [
            jax.ShapeDtypeStruct((groups, slab.shape[0], SUBS, LANES), jnp.float32),
            jax.ShapeDtypeStruct((3, jitter.shape[1]), jnp.int32),
        ],
        in_specs=[pl.BlockSpec(memory_space=pltpu.HBM)] * 4,
        out_specs=[vmem] * groups + [pl.BlockSpec(memory_space=pltpu.SMEM)],
        scratch_shapes=[
            pltpu.VMEM(slab.shape, jnp.float32),
            pltpu.SMEM(paths.shape, jnp.float32),
            pltpu.SMEM(jitter.shape, jnp.int32),
            pltpu.SMEM(steps.shape, jnp.float32),
            pltpu.SemaphoreType.DMA((4,)),
        ],
        name="terms",
    )(slab, paths, jitter, steps)
    return out[: groups - 1], out[groups - 1], out[groups]


def own_kernel(slab, paths, tables, term, kept):
    group = lax.axis_index("blk")
    for i, r, c in blocks_of(*slab.shape[1:]):
        term[i] = term_of(slab, paths, group, group, r, c)
    for i in range(tables.shape[0]):
        kept[i] = tables[i]


def own_term(slab, paths, patch):
    vmem = pl.BlockSpec(memory_space=pltpu.VMEM)
    tables = dft_tables(patch)
    return pl.pallas_call(
        own_kernel,
        out_shape=(listed(slab), jax.ShapeDtypeStruct(tables.shape, tables.dtype)),
        in_specs=[vmem, pl.BlockSpec(memory_space=pltpu.SMEM), vmem],
        out_specs=(vmem, vmem),
        compiler_params=pltpu.CompilerParams(vmem_limit_bytes=8 * 1024 * 1024),
        cost_estimate=pl.CostEstimate(flops=2**24, bytes_accessed=2**20, transcendentals=0),
        name="own",
    )(slab, paths, tables)


def update_kernel(slab, factors, *refs):
    grads, out = refs[:-1], refs[-1]
    layers, rows, cols = slab.shape
    for layer in range(layers):
        for i, r, c in blocks_of(rows, cols):
            value = slab[layer, r : r + SUBS, c : c + LANES]
            for step, grad in enumerate(grads):
                value = value - factors[step, layer] * grad[i]
            out[layer, r : r + SUBS, c : c + LANES] = value


def updated(slab, factors, grads):
    vmem = pl.BlockSpec(memory_space=pltpu.VMEM)
    return pl.pallas_call(
        update_kernel,
        out_shape=jax.ShapeDtypeStruct(slab.shape, slab.dtype),
        in_specs=[vmem] * (2 + len(grads)),
        out_specs=vmem,
        compiler_params=pltpu.CompilerParams(vmem_limit_bytes=8 * 1024 * 1024),
        cost_estimate=pl.CostEstimate(flops=2**24, bytes_accessed=2**20, transcendentals=0),
        name="update",
    )(slab, factors, *grads)


FLAGS = ("second", "lower", "up2", "dn2", "relay")


def prepare_kernel(number, scalars, probe, rolled, frames, twice):
    patch = probe.shape[1]
    for half in range(2):
        for part in range(2):
            twice[part, half * patch : (half + 1) * patch, :] = probe[part]
    for p in range(number):
        _, corner = window_place(p, patch)
        shift = corner + scalars[1, p]
        top = ROWS_DEV // 4 + scalars[0, p]
        start = patch - top
        for part in range(2):
            value = pltpu.roll(twice[part, pl.ds(start, patch), :], shift, 1)
            rolled[p * patch : (p + 1) * patch, part * LANES : (part + 1) * LANES] = value
        frames[p] = jnp.full((SUBS, LANES), shift, jnp.int32)
        frames[number + p] = jnp.full((SUBS, LANES), top, jnp.int32)
    for i in range(len(FLAGS)):
        frames[2 * number + i] = jnp.full((SUBS, LANES), scalars[2, i], jnp.int32)


def prepared(scalars, probe):
    number, patch = scalars.shape[1], probe.shape[1]
    vmem = pl.BlockSpec(memory_space=pltpu.VMEM)
    return pl.pallas_call(
        functools.partial(prepare_kernel, number),
        out_shape=(
            jax.ShapeDtypeStruct((number * patch, 2 * LANES), jnp.float32),
            jax.ShapeDtypeStruct((2 * number + len(FLAGS), SUBS, LANES), jnp.int32),
        ),
        in_specs=[pl.BlockSpec(memory_space=pltpu.SMEM), vmem],
        out_specs=(vmem, vmem),
        scratch_shapes=[pltpu.VMEM((2, 2 * patch, patch), jnp.float32)],
        compiler_params=pltpu.CompilerParams(vmem_limit_bytes=16 * 1024 * 1024),
        cost_estimate=pl.CostEstimate(flops=2**27, bytes_accessed=2**22, transcendentals=0),
        name="prepare",
    )(scalars, probe)


def flag_of(frames, name):
    return frames[frames.shape[0] - len(FLAGS) + FLAGS.index(name)] == 1


def frame_masks(frames, number, p):
    lane = lax.broadcasted_iota(jnp.int32, (SUBS, LANES), 1)
    sub = lax.broadcasted_iota(jnp.int32, (SUBS, LANES), 0)
    near = ROWS_DEV // 4 + JIT
    return lane >= frames[p], [sub + k * SUBS >= frames[number + p] for k in range(near // SUBS)]


def object_at(ref, first_block, row_block, p, patch, tiles, after):
    tile, _ = window_place(p, patch)
    first = first_block + row_block * tiles + tile
    left = ref[first] if tile >= 0 else 0.0
    right = ref[first + 1] if tile + 1 < tiles else 0.0
    return jnp.where(after, left, right)


def put_wave(wave, rolled, row, source, real, imag):
    a, b = rolled[pl.ds(source, SUBS), :LANES], rolled[pl.ds(source, SUBS), LANES:]
    wave[row : row + SUBS, :LANES] = a * real - b * imag
    wave[row : row + SUBS, LANES:] = a * imag + b * real


def against(high, low, t_high, t_low):
    left = jnp.concatenate([high, low, high], 1)
    return lax.dot(left, jnp.concatenate([t_high, t_high, t_low], 0), preferred_element_type=jnp.float32)


def onto(t_high, t_low, high, low):
    right = jnp.concatenate([high, low, high], 0)
    return lax.dot(jnp.concatenate([t_high, t_high, t_low], 1), right, preferred_element_type=jnp.float32)


def side_rows():
    second = lax.rem(lax.axis_index("wide"), 2)
    upper, lower = ROWS_DEV, 3 * ROWS_DEV
    return jnp.where(second == 1, upper, lower), jnp.where(second == 1, lower, upper)


def ahead_kernel(frames, own, mate, pair, next_pair, rolled, tables, wave, mid, real, imag):
    blocks = own.shape[0]
    patch = rolled.shape[1] // 2
    number = rolled.shape[0] // patch
    tiles = blocks * SUBS // ROWS_DEV
    steps = ROWS_DEV // SUBS
    lower = flag_of(frames, "lower")
    up2_ok = jnp.where(flag_of(frames, "up2"), 1.0, 0.0)
    dn2_ok = jnp.where(flag_of(frames, "dn2"), 1.0, 0.0)
    unused = ROWS_DEV // 4 // SUBS * tiles
    for i in range(blocks):
        if i >= unused:
            s, c = sin_cos(jnp.where(lower, pair[i], next_pair[i]))
            real[i], imag[i] = c * up2_ok, s * up2_ok
        if i < blocks - unused:
            s, c = sin_cos(jnp.where(lower, next_pair[i], pair[i]))
            real[blocks + i], imag[blocks + i] = c * dn2_ok, s * dn2_ok
        s, c = sin_cos(own[i])
        real[2 * blocks + i], imag[2 * blocks + i] = c, s
        s, c = sin_cos(mate[i])
        real[3 * blocks + i], imag[3 * blocks + i] = c, s

    mate_row, _ = side_rows()
    near = ROWS_DEV // 4 + JIT
    t_high, t_low = tables[0], tables[1]
    for p in range(number):
        after, below = frame_masks(frames, number, p)
        place = (p, patch, tiles, after)
        for k in range(steps):
            row = k * SUBS
            parts = []
            for ref in (real, imag):
                if row + SUBS <= ROWS_DEV // 4:
                    parts.append(object_at(ref, blocks, k, *place))
                elif row < near:
                    up = object_at(ref, 0, k, *place)
                    parts.append(jnp.where(below[k], up, object_at(ref, blocks, k, *place)))
                else:
                    parts.append(object_at(ref, 0, k, *place))
            put_wave(wave, rolled, p * patch + row, p * patch + row, *parts)
            parts = [object_at(ref, 2 * blocks, k, *place) for ref in (real, imag)]
            row += p * patch + 2 * ROWS_DEV
            put_wave(wave, rolled, row, row, *parts)
            row = k * SUBS
            parts = [object_at(ref, 3 * blocks, k, *place) for ref in (real, imag)]
            source = pl.multiple_of(p * patch + mate_row + row, SUBS)
            put_wave(wave, rolled, p * patch + ROWS_DEV + row, source, *parts)

    here = 3 * ROWS_DEV
    for p in range(0, number, TALL):
        windows = range(p, min(p + TALL, number))
        value = jnp.concatenate([wave[q * patch : q * patch + here, :] for q in windows], 0)
        out = against(*parts_of(value), t_high, t_low)
        for i, q in enumerate(windows):
            mid[q * patch : q * patch + here, :] = out[i * here : (i + 1) * here]


def ahead(frames, own, mate, pair, next_pair, rolled, tables):
    vmem = pl.BlockSpec(memory_space=pltpu.VMEM)
    out = jax.ShapeDtypeStruct(rolled.shape, jnp.float32)
    scratch = pltpu.VMEM((4 * own.shape[0], SUBS, LANES), jnp.float32)
    return pl.pallas_call(
        ahead_kernel,
        out_shape=(out, out),
        in_specs=[vmem] * 7,
        out_specs=(vmem, vmem),
        scratch_shapes=[scratch, scratch],
        compiler_params=pltpu.CompilerParams(vmem_limit_bytes=24 * 1024 * 1024),
        cost_estimate=pl.CostEstimate(flops=2**27, bytes_accessed=2**22, transcendentals=0),
        name="ahead",
    )(frames, own, mate, pair, next_pair, rolled, tables)


def strip_kernel(
    frames,
    wave,
    mid,
    relay,
    rolled,
    measured,
    tables,
    mine,
    to_mate,
    by_pair,
    by_next,
    misfit,
    real,
    imag,
    side_wave,
    side_mid,
    back,
    terms,
):
    number, patch, _ = measured.shape
    rows = ROWS_DEV
    blocks = relay.shape[0]
    tiles = blocks * SUBS // rows
    steps = patch // SUBS
    near = ROWS_DEV // 4 + JIT
    is_second = flag_of(frames, "second")
    is_lower = flag_of(frames, "lower")
    fwd_high, fwd_low, inv_high, inv_low = (tables[i] for i in range(4))

    relay_ok = jnp.where(flag_of(frames, "relay"), 1.0, 0.0)
    for i in range(blocks):
        s, c = sin_cos(relay[i])
        real[i], imag[i] = c * relay_ok, s * relay_ok
    _, relay_row = side_rows()
    for p in range(number):
        after, _ = frame_masks(frames, number, p)
        for k in range(rows // SUBS):
            parts = [object_at(ref, 0, k, p, patch, tiles, after) for ref in (real, imag)]
            source = pl.multiple_of(p * patch + relay_row + k * SUBS, SUBS)
            put_wave(side_wave, rolled, p * rows + k * SUBS, source, *parts)
    for p in range(0, number, SIDE):
        span = slice(p * rows, min(p + SIDE, number) * rows)
        side_mid[span, :] = against(*parts_of(side_wave[span, :]), fwd_high, fwd_low)
    second = relay_row > 2 * rows

    def window_rows(whole, side, p):
        at = p * patch
        mates, others = whole[at + rows : at + 2 * rows, :], side[p * rows : (p + 1) * rows, :]
        upper, lower = jnp.where(second, mates, others), jnp.where(second, others, mates)
        return jnp.concatenate([whole[at : at + rows, :], upper, whole[at + 2 * rows : at + 3 * rows, :], lower], 0)

    def upright(value):
        count = value.shape[0] // patch
        parts = [
            jnp.concatenate([value[i * patch : (i + 1) * patch, lanes] for i in range(count)], 1)
            for lanes in (slice(0, LANES), slice(LANES, 2 * LANES))
        ]
        return jnp.concatenate(parts, 0)

    total = jnp.zeros((SUBS, LANES), jnp.float32)
    for p in range(0, number, BROAD):
        count = min(BROAD, number - p)
        high, low = parts_of(upright(jnp.concatenate([window_rows(mid, side_mid, p + i) for i in range(count)], 0)))
        spectrum = onto(inv_high, inv_low, high, low)
        real, imag = spectrum[:patch], spectrum[patch:]
        target = jnp.concatenate([measured[p + i] for i in range(count)], 1).astype(jnp.float32)
        power = real * real + imag * imag
        inverse = lax.rsqrt(jnp.maximum(power, 1e-30))
        error = power * inverse - target
        square = error * error
        for k in range(steps):
            for half in range(count):
                total += square[k * SUBS : (k + 1) * SUBS, half * LANES : (half + 1) * LANES]
        ratio = target * jnp.minimum(inverse, FLOOR_RATIO)
        high, low = parts_of(jnp.concatenate([ratio * real, ratio * imag], 0))
        undone = onto(fwd_high, fwd_low, high, low)
        for half in range(count):
            row = (p + half) * patch
            lanes = slice(half * LANES, (half + 1) * LANES)
            back[row : row + patch, :LANES] = undone[:patch, lanes]
            back[row : row + patch, LANES:] = undone[patch:, lanes]
    misfit[0] = total

    for p in range(0, number, TALL):
        span = slice(p * patch, min(p + TALL, number) * patch)
        high, low = parts_of(back[span, :])
        out = against(high, low, inv_high, inv_low)
        windows = range(p, min(p + TALL, number))
        w = jnp.concatenate([window_rows(wave, side_wave, q) for q in windows], 0)
        terms[span, :] = w[:, :LANES] * out[:, LANES:] - w[:, LANES:] * out[:, :LANES]

    grads = {}
    for t in range(tiles):
        meets = []
        for p in range(number):
            tile, _ = window_place(p, patch)
            if t in (tile, tile + 1):
                after, below = frame_masks(frames, number, p)
                meets.append((p, after if t == tile else jnp.logical_not(after), below))
        for k in range(steps):
            row = k * SUBS
            here = there = None
            for p, mask, below in meets:
                term = jnp.where(mask, terms[p * patch + row : p * patch + row + SUBS, :], 0.0)
                if row + SUBS <= ROWS_DEV // 4:
                    there = term if there is None else there + term
                elif row < near:
                    kept = jnp.where(below[k], term, 0.0)
                    here = kept if here is None else here + kept
                    there = (term - kept) if there is None else there + (term - kept)
                else:
                    here = term if here is None else here + term
            grads[k, t] = here
            grads[k + steps, t] = there

    def add_to(slot, r, t):
        value = grads.get((slot * (rows // SUBS) + r // SUBS, t))
        return jnp.zeros((SUBS, LANES), jnp.float32) if value is None else value

    for i, r, c in blocks_of(rows, tiles * LANES):
        up2, up1, here, dn1, dn2 = (add_to(slot, r, c // LANES) for slot in range(5))
        mine[i] = here
        to_mate[i] = jnp.where(is_second, up1, dn1)
        to_mate[blocks + i] = jnp.where(is_second, dn1, up1)
        by_pair[i] = jnp.where(is_lower, up2, dn2)
        by_next[i] = jnp.where(is_lower, dn2, up2)


def strip_gradient(frames, wave, mid, relay, rolled, measured, tables):
    number, patch, _ = measured.shape
    blocks = relay.shape[0]
    vmem = pl.BlockSpec(memory_space=pltpu.VMEM)

    def block_list(count):
        return jax.ShapeDtypeStruct((count, SUBS, LANES), jnp.float32)

    side = pltpu.VMEM((number * ROWS_DEV, 2 * LANES), jnp.float32)
    return pl.pallas_call(
        strip_kernel,
        out_shape=tuple(block_list(n) for n in (blocks, 2 * blocks, blocks, blocks, 1)),
        in_specs=[vmem] * 7,
        out_specs=(vmem,) * 5,
        scratch_shapes=[
            pltpu.VMEM((blocks, SUBS, LANES), jnp.float32),
            pltpu.VMEM((blocks, SUBS, LANES), jnp.float32),
            side,
            side,
            pltpu.VMEM((number * patch, 2 * LANES), jnp.float32),
            pltpu.VMEM((number * patch, LANES), jnp.float32),
        ],
        compiler_params=pltpu.CompilerParams(vmem_limit_bytes=40 * 1024 * 1024),
        cost_estimate=pl.CostEstimate(
            flops=24 * number * patch**3 * 4, bytes_accessed=4 * number * patch * patch, transcendentals=0
        ),
        name="strip",
    )(frames, wave, mid, relay, rolled, measured, tables)


def permuted(value, axis, target):
    count = lax.axis_size(axis)
    pairs = [(i, target(i)) for i in range(count) if 0 <= target(i) < count]
    return lax.ppermute(value, axis, pairs)


def with_mate(value):
    return permuted(value, "wide", lambda i: i ^ 1)


def with_pair(value):
    return permuted(value, "wide", lambda i: i ^ 2)


def across(value):
    count = lax.axis_size("wide")

    def target(i):
        j = i + 2 if i // 2 % 2 else i - 2
        return j if 0 <= j < count else i ^ 1

    return permuted(value, "wide", target)


def joined(value, axis, steps):
    for step in steps:
        value = value + permuted(value, axis, lambda i: i ^ step)
    return value


def program(volume, path_lengths, probe, measured, jitter, step_sizes):
    groups = lax.axis_size("blk")
    column = lax.axis_index("wide")
    columns = lax.axis_size("wide")
    slab = volume[0]

    def to_group(value, step):
        return lax.ppermute(value, "blk", [(i, (i + step) % groups) for i in range(groups)])

    terms, factors, scalars = slab_terms(slab, path_lengths, jitter[:, 0, 0], step_sizes, groups)
    own, tables = own_term(slab, path_lengths, probe.shape[-1])
    for step in range(1, groups):
        own = own + to_group(terms[step - 1], step)

    even = column % 2 == column // 2 % 2
    next_pair = across(own)
    pair = with_pair(own)
    mate = with_mate(own)
    rolled, frames = prepared(scalars, probe)
    relay = with_mate(jnp.where(even, pair, next_pair))
    wave, mid = ahead(frames, own, mate, pair, next_pair, rolled, tables)
    blocks = own.shape[0]
    mine, to_mate, by_pair, by_next, local = strip_gradient(frames, wave, mid, relay, rolled, measured[0, 0], tables)
    got = with_mate(to_mate)
    if groups != 2:
        local = joined(local, "blk", [2**k for k in range(groups.bit_length() - 1)])
    local = joined(local, "wide", [2])
    mine = mine + got[:blocks]
    passed = got[blocks:]
    zero = jnp.zeros_like(passed)
    from_pair = with_pair(by_pair + jnp.where(even, passed, zero))
    from_next = across(by_next + jnp.where(even, zero, passed))
    local = joined(local, "wide", [1])
    local = joined(local, "wide", [8] + [2**k for k in range(4, columns.bit_length() - 1)])
    gradient = mine + (from_next + from_pair)
    grads = [gradient]
    if groups == 2:
        grads.append(to_group(jnp.concatenate([gradient, local], 0), 1))
        sums = [local, permuted(local, "wide", lambda i: i ^ 4)]
        pairs = [(i, (i + columns) % (2 * columns) ^ 4) for i in range(2 * columns)]
        sums.append(lax.ppermute(local, ("blk", "wide"), pairs))
    else:
        for step in range(1, groups):
            grads.append(to_group(gradient, step))
        sums = [joined(local, "wide", [4])]
    new = updated(slab, factors, grads)
    if groups == 2:
        sums = [(sums[0] + sums[1]) + (grads[1][blocks:] + sums[2])]
    return (new[None], jnp.sum(sums[0]))


def solution(mesh):
    in_specs = (
        P("blk", None, "wide", None),
        P(),
        P(),
        P("blk", "wide", None, None, None),
        P(None, "blk", "wide", None),
        P(),
    )
    out_specs = (P("blk", None, "wide", None), P())
    return jax.shard_map(program, mesh=mesh, in_specs=in_specs, out_specs=out_specs, check_vma=False)
```
